8 devices in a mesh: data: 1 (over z), tp: 8 (over y, x, core).
Axes of the slice: x: 2, y: 2, z: 1, core: 2. Of those that a mesh axis runs over, the one named last changes fastest.
Arguments:
- x_tokens: bfloat16 [4096, 1152], P(('data', 'tp'))
- ln_gamma: float32 [1152], replicated
- w_qkv: bfloat16 [1152, 16, 216], P(None, 'tp')
- w_out: bfloat16 [16, 72, 1152], P('tp')
- w_up: bfloat16 [1152, 4608], P(None, 'tp')
- w_down: bfloat16 [4608, 1152], P('tp')
Outputs:
- output: bfloat16 [4096, 1152], P(('data', 'tp'))
All inputs are finite; a program needn't handle non-finite values.
Results may differ from the reference program's by a relative error of at most 0.00218372.
Values are sent between devices in bfloat16 or wider.
A program may use at most 1 GiB of HBM per device.

```python
import math
import jax
import jax.numpy as jnp
from jax import lax

SEQ_LEN = 4096
MODEL_DIM = 1152
FF_DIM = 4608
NUM_HEADS = 16
HEAD_DIM = MODEL_DIM // NUM_HEADS
BLOCK_ROWS = min(SEQ_LEN, 256)
N_BLOCKS = SEQ_LEN // BLOCK_ROWS
ATTN_SCALE = HEAD_DIM ** -0.5
LN_EPS = 1e-6
QK_GAIN = max(math.log(SEQ_LEN) - 2.0, 1.0) ** 0.25


def setup_inputs(seed: int = 0, part: int = 0) -> dict:
    rand_keys = jax.random.split(jax.random.key(seed), 6)
    tokens = jax.random.normal(jax.random.fold_in(rand_keys[0], part), (SEQ_LEN, MODEL_DIM), jnp.float32)
    ln_gain = 1.0 + 0.5 * jax.random.normal(rand_keys[1], (MODEL_DIM,), jnp.float32)
    qkv_gain = jnp.array([QK_GAIN, QK_GAIN, 1.0], jnp.float32).reshape(1, 1, 3, 1)
    w_qkv = jax.random.normal(rand_keys[2], (MODEL_DIM, NUM_HEADS, 3, HEAD_DIM), jnp.float32) * qkv_gain * MODEL_DIM ** -0.5
    w_out = jax.random.normal(rand_keys[3], (NUM_HEADS, HEAD_DIM, MODEL_DIM), jnp.float32) * (2.0 * MODEL_DIM ** -0.5)
    w_up = jax.random.normal(rand_keys[4], (MODEL_DIM, FF_DIM), jnp.float32) * MODEL_DIM ** -0.5
    w_down = jax.random.normal(rand_keys[5], (FF_DIM, MODEL_DIM), jnp.float32) * (1.5 * FF_DIM ** -0.5)
    return {
        "x_tokens": tokens.astype(jnp.bfloat16),
        "ln_gamma": ln_gain,
        "w_qkv": w_qkv.reshape(MODEL_DIM, NUM_HEADS, 3 * HEAD_DIM).astype(jnp.bfloat16),
        "w_out": w_out.astype(jnp.bfloat16),
        "w_up": w_up.astype(jnp.bfloat16),
        "w_down": w_down.astype(jnp.bfloat16),
    }


def layer_norm(row_vals, ln_gain):
    row_mean = jnp.mean(row_vals, axis=-1, keepdims=True)
    centered = row_vals - row_mean
    row_var = jnp.mean(centered * centered, axis=-1, keepdims=True)
    return centered * lax.rsqrt(row_var + LN_EPS) * ln_gain


def reference(x_tokens, ln_gamma, w_qkv, w_out, w_up, w_down):
    residual = x_tokens.astype(jnp.float32)
    normed = layer_norm(residual, ln_gamma).astype(jnp.bfloat16)

    def head_step(attn_acc, head_weights):
        wqkv_head, wout_head = head_weights
        qkv_rows = jnp.dot(normed, wqkv_head, preferred_element_type=jnp.float32).astype(jnp.bfloat16)
        query_rows = qkv_rows[:, :HEAD_DIM]
        key_trans = qkv_rows[:, HEAD_DIM:2 * HEAD_DIM].T
        value_rows = qkv_rows[:, 2 * HEAD_DIM:]

        def query_block(query_blk):
            scores = jnp.dot(query_blk, key_trans, preferred_element_type=jnp.float32) * ATTN_SCALE
            row_max = jnp.max(scores, axis=-1, keepdims=True)
            exp_scores = jnp.exp(scores - row_max)
            exp_sum = jnp.sum(exp_scores, axis=-1, keepdims=True)
            block_out = jnp.dot(exp_scores.astype(jnp.bfloat16), value_rows, preferred_element_type=jnp.float32)
            return (block_out / exp_sum).astype(jnp.bfloat16)

        head_out = lax.map(query_block, query_rows.reshape(N_BLOCKS, BLOCK_ROWS, HEAD_DIM)).reshape(SEQ_LEN, HEAD_DIM)
        return attn_acc + jnp.dot(head_out, wout_head, preferred_element_type=jnp.float32), None

    attn_init = jnp.zeros((SEQ_LEN, MODEL_DIM), jnp.float32)
    attn_sum = lax.scan(head_step, attn_init, (jnp.moveaxis(w_qkv, 1, 0), w_out))[0]

    def mlp_block(row_blk):
        pre_act = jnp.dot(row_blk, w_up, preferred_element_type=jnp.float32)
        hidden = jax.nn.gelu(pre_act, approximate=True).astype(jnp.bfloat16)
        return jnp.dot(hidden, w_down, preferred_element_type=jnp.float32)

    mlp_sum = lax.map(mlp_block, normed.reshape(N_BLOCKS, BLOCK_ROWS, MODEL_DIM)).reshape(SEQ_LEN, MODEL_DIM)
    return (residual + attn_sum + mlp_sum).astype(jnp.bfloat16)
```

```python
import math
import jax
import jax.numpy as jnp
from jax import lax
from jax.experimental import pallas as pl
from jax.experimental.pallas import tpu as pltpu
from jax.sharding import PartitionSpec as P

LN_EPS = 1e-6
LANES = 128
ROWS = 256
UNITS = 8
F32 = jnp.float32
BF16 = jnp.bfloat16


def gelu_tanh(v):
    return jax.nn.gelu(v, approximate=True)


def block_kernel(head_dim, head_rows, x_hbm, gamma_ref, wqkv_hbm, wout_hbm, w1_hbm, w2_hbm, y_ref,
                 x_ref, xg, wqkv, wout, w1, w2, q_all, k_all, v_all, part, recv, s_even, s_odd, m_even, m_odd, o_t,
                 load_sem, wsend, wrecv, gsend, grecv, kvsend, kvrecv, rsend, rrecv):
    me = lax.axis_index("tp")
    core = lax.rem(me, 2)
    chip_x = lax.rem(me // 2, 2)
    chip_y = me // 4
    sib = me + 1 - 2 * core
    x_nbr = me + 2 - 4 * chip_x
    y_nbr = me + 4 - 8 * chip_y

    def remote(src, dst, send, rcv, dev):
        return pltpu.make_async_remote_copy(src_ref=src, dst_ref=dst, send_sem=send, recv_sem=rcv,
                                            device_id={"tp": dev}, device_id_type=pl.DeviceIdType.MESH)

    own_out = wout.at[pl.ds(pl.multiple_of(core * 2 * head_rows, 2 * head_rows), 2 * head_rows)]

    loads = [
        pltpu.make_async_copy(x_hbm, x_ref, load_sem.at[0]),
        pltpu.make_async_copy(wqkv_hbm, wqkv.at[core], load_sem.at[1]),
        pltpu.make_async_copy(w1_hbm, w1.at[core], load_sem.at[2]),
        pltpu.make_async_copy(w2_hbm, w2.at[core], load_sem.at[3]),
        pltpu.make_async_copy(wout_hbm, own_out, load_sem.at[4]),
    ]
    for cp in loads:
        cp.start()

    barrier = pltpu.get_barrier_semaphore()
    for dev in (sib, x_nbr, y_nbr):
        pl.semaphore_signal(barrier, inc=1, device_id={"tp": dev}, device_id_type=pl.DeviceIdType.MESH)

    loads[0].wait()
    for half in (0, 1):
        rows = x_ref[pl.ds(half * ROWS, ROWS), :].astype(F32)
        mean = jnp.mean(rows, axis=-1, keepdims=True)
        cent = rows - mean
        var = jnp.mean(cent * cent, axis=-1, keepdims=True)
        xg[half] = (cent * lax.rsqrt(var + LN_EPS) * gamma_ref[...]).astype(BF16)

    pl.semaphore_wait(barrier, 3)

    def gather_copy(src, dst, idx, dev):
        return remote(xg.at[src], xg.at[dst], gsend.at[idx], grecv.at[idx], dev)

    g_copies = [
        gather_copy(0, 2, 0, y_nbr),
        gather_copy(1, 3, 1, x_nbr),
        gather_copy(0, 4, 2, x_nbr),
        gather_copy(1, 5, 3, y_nbr),
        gather_copy(2, 6, 4, x_nbr),
        gather_copy(3, 7, 5, y_nbr),
    ]
    for cp in g_copies[:4]:
        cp.start()
    w_copies = [
        remote(wqkv_hbm, wqkv.at[core], wsend.at[0], wrecv.at[0], sib),
        remote(w1_hbm, w1.at[core], wsend.at[1], wrecv.at[1], sib),
        remote(w2_hbm, w2.at[core], wsend.at[2], wrecv.at[2], sib),
        remote(wout_hbm, own_out, wsend.at[3], wrecv.at[3], sib),
    ]
    for cp in w_copies:
        cp.start()
    for cp in loads[1:]:
        cp.wait()
    for cp in w_copies:
        cp.wait_recv()

    def kv_copies(unit):
        return (
            remote(k_all.at[unit], k_all.at[UNITS + unit], kvsend.at[0, unit], kvrecv.at[0, unit], sib),
            remote(v_all.at[unit], v_all.at[UNITS + unit], kvsend.at[1, unit], kvrecv.at[1, unit], sib),
        )

    def project(unit, _):
        @pl.when(unit == 2)
        def _():
            g_copies[0].wait_recv()
            g_copies[4].start()
            g_copies[1].wait_recv()
            g_copies[5].start()

        @pl.when(unit == 4)
        def _():
            g_copies[2].wait_recv()
            g_copies[3].wait_recv()

        @pl.when(unit == 6)
        def _():
            g_copies[4].wait_recv()
            g_copies[5].wait_recv()

        rows = xg[unit]
        for s in (0, 1):
            qkv = jnp.dot(rows, wqkv[s], preferred_element_type=F32)
            for hh in (0, 1):
                h = 2 * s + hh
                base = hh * 3 * LANES
                q_all[unit, h] = qkv[:, base:base + LANES].astype(BF16)
                k_all[unit, h] = qkv[:, base + LANES:base + 2 * LANES].astype(BF16)
                v_t = jnp.transpose(qkv[:, base + 2 * LANES:base + 3 * LANES])
                v_all[unit, h] = v_t[:head_rows].astype(BF16)
        for cp in kv_copies(unit):
            cp.start()
        total = None
        for s in (0, 1):
            hidden = gelu_tanh(jnp.dot(rows, w1[s], preferred_element_type=F32)).astype(BF16)
            term = jnp.dot(hidden, w2[s], preferred_element_type=F32)
            total = term if total is None else total + term
        part[unit] = total
        return 0

    lax.fori_loop(0, UNITS, project, 0)

    def kv_wait(unit, _):
        for cp in kv_copies(unit):
            cp.wait()
        return 0

    lax.fori_loop(0, UNITS, kv_wait, 0)

    exp_scale = (head_dim ** -0.5) * math.log2(math.e)
    groups = ROWS // 8

    def score_chunk(c, unit, h, q, s_ref):
        s = lax.dot_general(k_all[c, h], q, (((1,), (1,)), ((), ())), preferred_element_type=F32)
        s_ref[pl.ds(c * ROWS, ROWS), :] = s
        return jnp.max(s.reshape(groups, 8, ROWS), axis=0)

    def scores(unit, h, s_ref, m_ref):
        q = q_all[unit, h]
        m = None
        for c in range(2 * UNITS):
            mc = score_chunk(c, unit, h, q, s_ref)
            m = mc if m is None else jnp.maximum(m, mc)
        m_ref[...] = m

    def finish(h, s_ref, m_ref, unit_n, h_n, s_next, m_next):
        q_n = q_all[unit_n, h_n]
        m = jnp.max(m_ref[...], axis=0, keepdims=True)
        acc = None
        total = None
        m_n = None
        for c in range(2 * UNITS):
            mc = score_chunk(c, unit_n, h_n, q_n, s_next)
            m_n = mc if m_n is None else jnp.maximum(m_n, mc)
            e = jnp.exp2((s_ref[pl.ds(c * ROWS, ROWS), :] - m) * exp_scale)
            tc = jnp.sum(e.reshape(groups, 8, ROWS), axis=0)
            total = tc if total is None else total + tc
            pv = jnp.dot(v_all[c, h], e.astype(BF16), preferred_element_type=F32)
            acc = pv if acc is None else acc + pv
        m_next[...] = m_n
        denom = jnp.sum(total, axis=0, keepdims=True)
        start = pl.multiple_of(h * head_rows, head_rows)
        o_t[pl.ds(start, head_rows), :] = (acc / denom).astype(BF16)

    def unit_of(i):
        return 2 * (3 - i // 2) + lax.rem(i, 2)

    def reduce_copy(idx, src, dev):
        return remote(part.at[src], recv.at[idx], rsend.at[idx], rrecv.at[idx], dev)

    r_copies = [
        reduce_copy(0, 6, x_nbr),
        reduce_copy(1, 7, y_nbr),
        reduce_copy(2, 4, x_nbr),
        reduce_copy(3, 5, y_nbr),
        reduce_copy(4, 2, y_nbr),
        reduce_copy(5, 3, x_nbr),
    ]

    scores(unit_of(0), 0, s_even, m_even)

    def attend(i, _):
        unit = unit_of(i)
        unit_next = unit_of(lax.rem(i + 1, UNITS))

        def pair(p, _):
            finish(2 * p, s_even, m_even, unit, 2 * p + 1, s_odd, m_odd)
            after = unit + p * (unit_next - unit)
            finish(2 * p + 1, s_odd, m_odd, after, 2 - 2 * p, s_even, m_even)
            return 0

        lax.fori_loop(0, 2, pair, 0)
        part[unit] += lax.dot_general(o_t[...], wout[...], (((0,), (0,)), ((), ())), preferred_element_type=F32)
        for step in range(6):
            @pl.when(i == step)
            def _():
                if step >= 4:
                    r_copies[step - 4].wait_recv()
                    part[step - 2] += recv[step - 4]
                r_copies[step].start()
        return 0

    lax.fori_loop(0, UNITS, attend, 0)

    for half, first, second in ((0, 2, 4), (1, 3, 5)):
        r_copies[first].wait_recv()
        r_copies[second].wait_recv()
        span = pl.ds(half * ROWS, ROWS)
        y_ref[span, :] = (x_ref[span, :].astype(F32) + part[half] + recv[first] + recv[second]).astype(BF16)
    for cp in g_copies + w_copies + r_copies:
        cp.wait_send()


def solution(mesh):
    def local_block(x_loc, ln_gamma, w_qkv, w_out, w_up, w_down):
        model_dim = x_loc.shape[1]
        heads = w_qkv.shape[1]
        head_dim = w_qkv.shape[2] // 3
        ff = w_up.shape[1]
        head_rows = -(-head_dim // 16) * 16
        wqkv = jnp.pad(w_qkv.reshape(model_dim, heads, 3, head_dim), ((0, 0), (0, 0), (0, 0), (0, LANES - head_dim)))
        wqkv = wqkv.reshape(model_dim, heads * 3 * LANES)
        wout = jnp.pad(w_out, ((0, 0), (0, head_rows - head_dim), (0, 0))).reshape(heads * head_rows, model_dim)
        any_spec = pl.BlockSpec(memory_space=pl.ANY)
        vmem_spec = pl.BlockSpec(memory_space=pltpu.VMEM)
        all_heads = 2 * heads
        keys = 2 * UNITS * ROWS
        dma = pltpu.SemaphoreType.DMA
        kern = lambda *refs: block_kernel(head_dim, head_rows, *refs)
        return pl.pallas_call(
            kern,
            out_shape=jax.ShapeDtypeStruct(x_loc.shape, BF16),
            in_specs=[any_spec, vmem_spec, any_spec, any_spec, any_spec, any_spec],
            out_specs=vmem_spec,
            scratch_shapes=[
                pltpu.VMEM(x_loc.shape, BF16),
                pltpu.VMEM((UNITS, ROWS, model_dim), BF16),
                pltpu.VMEM((2,) + wqkv.shape, BF16),
                pltpu.VMEM((all_heads * head_rows, model_dim), BF16),
                pltpu.VMEM((2, model_dim, ff), BF16),
                pltpu.VMEM((2, ff, model_dim), BF16),
                pltpu.VMEM((UNITS, all_heads, ROWS, LANES), BF16),
                pltpu.VMEM((2 * UNITS, all_heads, ROWS, LANES), BF16),
                pltpu.VMEM((2 * UNITS, all_heads, head_rows, ROWS), BF16),
                pltpu.VMEM((UNITS, ROWS, model_dim), F32),
                pltpu.VMEM((6, ROWS, model_dim), F32),
                pltpu.VMEM((keys, ROWS), F32),
                pltpu.VMEM((keys, ROWS), F32),
                pltpu.VMEM((8, ROWS), F32),
                pltpu.VMEM((8, ROWS), F32),
                pltpu.VMEM((all_heads * head_rows, ROWS), BF16),
                dma((5,)), dma((4,)), dma((4,)), dma((6,)), dma((6,)),
                dma((2, UNITS)), dma((2, UNITS)), dma((6,)), dma((6,)),
            ],
            compiler_params=pltpu.CompilerParams(collective_id=0, has_side_effects=True, vmem_limit_bytes=67043328),
            name="parallel_block",
        )(x_loc, ln_gamma.reshape(1, model_dim), wqkv, wout, w_up, w_down)

    row_spec = P(("data", "tp"), None)
    return jax.shard_map(local_block, mesh=mesh, in_specs=(row_spec, P(None), P(None, "tp", None), P("tp", None, None), P(None, "tp"), P("tp", None)), out_specs=row_spec, check_vma=False)
```

```python
import functools
import math
import jax
import jax.numpy as jnp
from jax import lax
from jax.experimental import pallas as pl
from jax.experimental.pallas import tpu as pltpu
from jax.sharding import PartitionSpec as P

LN_EPS = 1e-6
LANES = 128
ROWS = 256
UNITS = 8
CHUNKS = 2 * UNITS
HEADS = 4
F32 = jnp.float32
BF16 = jnp.bfloat16
ROW_MAJOR = (((1,), (0,)), ((), ()))
BY_ROWS = (((1,), (1,)), ((), ()))
BY_COLS = (((0,), (0,)), ((), ()))


def dot(a, b, dims=ROW_MAJOR):
    return lax.dot_general(a, b, dims, preferred_element_type=F32)


def gelu_tanh(v):
    return jax.nn.gelu(v, approximate=True)


def block_kernel(head_dim, head_rows, x_hbm, gamma_ref, wqkv_hbm, wout_hbm, w1_hbm, w2_hbm, y_ref,
                 xg, xn, wqv, wk, wout, w1, w2, q_all, k_all, v_all, part, recv, s_even, s_odd, m_even, m_odd, o_t,
                 acc_st, m_st, l_st,
                 load_sem, wsend, wrecv, gsend, grecv, kvsend, kvrecv, rsend, rrecv):
    me = lax.axis_index("tp")
    core = lax.rem(me, 2)
    chip_x = lax.rem(me // 2, 2)
    chip_y = me // 4
    sib = me + 1 - 2 * core
    x_nbr = me + 2 - 4 * chip_x
    y_nbr = me + 4 - 8 * chip_y
    mesh_id = pl.DeviceIdType.MESH

    def remote(src, dst, send, rcv, dev):
        return pltpu.make_async_remote_copy(src_ref=src, dst_ref=dst, send_sem=send, recv_sem=rcv,
                                            device_id={"tp": dev}, device_id_type=mesh_id)

    wqv[:, :, head_rows - 16:, :] = jnp.zeros((2, HEADS, 16, wqv.shape[3]), BF16)
    wk[:, LANES - 64:, :] = jnp.zeros((HEADS, 64, wk.shape[2]), BF16)
    wout[:, head_rows - 16:, :] = jnp.zeros((HEADS, 16, wout.shape[2]), BF16)

    barrier = pltpu.get_barrier_semaphore()
    for dev in (sib, x_nbr, y_nbr):
        pl.semaphore_signal(barrier, inc=1, device_id={"tp": dev}, device_id_type=mesh_id)

    pairs = []
    for hh in (0, 1):
        h = 2 * core + hh
        real = pl.ds(0, head_dim)
        pairs += [
            (wqkv_hbm.at[hh, pl.ds(0, head_dim)], wqv.at[0, h, real]),
            (wqkv_hbm.at[hh, pl.ds(head_dim, head_dim)], wk.at[h, real]),
            (wqkv_hbm.at[hh, pl.ds(2 * head_dim, head_dim)], wqv.at[1, h, real]),
            (wout_hbm.at[hh], wout.at[h, real]),
        ]
    pairs += [(w1_hbm, w1.at[core]), (w2_hbm, w2.at[core])]
    loads = [pltpu.make_async_copy(x_hbm.at[pl.ds(half * ROWS, ROWS)], xg.at[half], load_sem.at[half]) for half in (0, 1)]
    loads += [pltpu.make_async_copy(src, dst, load_sem.at[2 + n]) for n, (src, dst) in enumerate(pairs)]
    for cp in loads:
        cp.start()

    pl.semaphore_wait(barrier, 3)

    def gather_copy(src, dst, idx, dev):
        return remote(src, xg.at[dst], gsend.at[idx], grecv.at[idx], dev)

    half_1, half_2 = x_hbm.at[pl.ds(0, ROWS)], x_hbm.at[pl.ds(ROWS, ROWS)]
    g_copies = [
        gather_copy(half_1, 2, 0, y_nbr),
        gather_copy(half_2, 3, 1, x_nbr),
        gather_copy(half_1, 4, 2, x_nbr),
        gather_copy(half_2, 5, 3, y_nbr),
        gather_copy(xg.at[2], 6, 4, x_nbr),
        gather_copy(xg.at[3], 7, 5, y_nbr),
    ]
    for cp in g_copies[:4]:
        cp.start()
    w_copies = [remote(src, dst, wsend.at[n], wrecv.at[n], sib) for n, (src, dst) in enumerate(pairs)]
    for cp in w_copies:
        cp.start()

    zero_rows = LANES - head_rows

    def clear(unit, _):
        q_all[unit, :, head_rows:, :] = jnp.zeros((HEADS, zero_rows, ROWS), BF16)
        return 0

    lax.fori_loop(0, UNITS, clear, 0)

    def kv_copies(unit):
        return (
            remote(k_all.at[unit], k_all.at[UNITS + unit], kvsend.at[0, unit], kvrecv.at[0, unit], sib),
            remote(v_all.at[unit], v_all.at[UNITS + unit], kvsend.at[1, unit], kvrecv.at[1, unit], sib),
        )

    def project(unit, _):
        rows = xg[unit].astype(F32)
        mean = jnp.mean(rows, axis=-1, keepdims=True)
        cent = rows - mean
        var = jnp.mean(cent * cent, axis=-1, keepdims=True)
        normed = (cent * lax.rsqrt(var + LN_EPS) * gamma_ref[...]).astype(BF16)
        xn[unit] = normed
        keys = dot(normed, wk[...].reshape(HEADS * LANES, -1), BY_ROWS)
        qv = dot(wqv[...].reshape(2 * HEADS * head_rows, -1), normed, BY_ROWS).astype(BF16)
        for h in range(HEADS):
            k_all[unit, h] = keys[:, h * LANES:(h + 1) * LANES].astype(BF16)
            q_all[unit, h, :head_rows] = qv[h * head_rows:(h + 1) * head_rows]
            v_all[unit, h] = qv[(HEADS + h) * head_rows:(HEADS + h + 1) * head_rows]
        for cp in kv_copies(unit):
            cp.start()
        return 0

    def mlp(unit, _):
        rows = xn[unit]
        total = None
        for s in (0, 1):
            hidden = gelu_tanh(dot(rows, w1[s], BY_ROWS)).astype(BF16)
            term = dot(hidden, w2[s])
            total = term if total is None else total + term
        part[unit] = total
        return 0

    def kv_wait(unit, _):
        for cp in kv_copies(unit):
            cp.wait()
        return 0

    exp_scale = (head_dim ** -0.5) * math.log2(math.e)
    groups = ROWS // 8

    def score_chunk(n, c, h, q, s_ref):
        s = dot(k_all[c, h], q)
        s_ref[pl.ds(n * ROWS, ROWS), :] = s
        return jnp.max(s.reshape(groups, 8, ROWS), axis=0)

    def finish(chunks, h, s_ref, m_ref, unit_n, h_n, s_next, m_next):
        q_n = q_all[unit_n, h_n]
        m = jnp.max(m_ref[...], axis=0, keepdims=True)
        acc = None
        total = None
        m_n = None
        for n, c in enumerate(chunks):
            mc = score_chunk(n, c, h_n, q_n, s_next)
            m_n = mc if m_n is None else jnp.maximum(m_n, mc)
            e = jnp.exp2((s_ref[pl.ds(n * ROWS, ROWS), :] - m) * exp_scale)
            tc = jnp.sum(e.reshape(groups, 8, ROWS), axis=0)
            total = tc if total is None else total + tc
            pv = dot(v_all[c, h], e.astype(BF16))
            acc = pv if acc is None else acc + pv
        m_next[...] = m_n
        return m, jnp.sum(total, axis=0, keepdims=True), acc

    def attend(count, unit_of, chunks, emit, after):
        q = q_all[unit_of(0), 0]
        m = None
        for n, c in enumerate(chunks):
            mc = score_chunk(n, c, 0, q, s_even)
            m = mc if m is None else jnp.maximum(m, mc)
        m_even[...] = m

        def one(i, _):
            unit = unit_of(i)
            unit_next = unit_of(lax.rem(i + 1, count))

            def pair(p, _):
                emit(i, 2 * p, *finish(chunks, 2 * p, s_even, m_even, unit, 2 * p + 1, s_odd, m_odd))
                follow = unit + p * (unit_next - unit)
                emit(i, 2 * p + 1, *finish(chunks, 2 * p + 1, s_odd, m_odd, follow, 2 - 2 * p, s_even, m_even))
                return 0

            lax.fori_loop(0, 2, pair, 0)
            after(i, unit)
            return 0

        lax.fori_loop(0, count, one, 0)

    def emit_state(i, h, m, total, acc):
        m_st[i, h] = jnp.broadcast_to(m, m_st.shape[2:])
        l_st[i, h] = jnp.broadcast_to(total, l_st.shape[2:])
        acc_st[i, h] = acc

    def emit_merged(i, h, m, total, acc):
        m_old = m_st[i, h][:1]
        top = jnp.maximum(m, m_old)
        a_new = jnp.exp2((m - top) * exp_scale)
        a_old = jnp.exp2((m_old - top) * exp_scale)
        denom = total * a_new + l_st[i, h][:1] * a_old
        o_t[h] = ((acc * a_new + acc_st[i, h] * a_old) / denom).astype(BF16)

    def emit_out(i, h, m, total, acc):
        o_t[h] = (acc / total).astype(BF16)

    def add_heads(unit):
        part[unit] += dot(o_t[...].reshape(HEADS * head_rows, ROWS), wout[...].reshape(HEADS * head_rows, -1), BY_COLS)

    def reduce_copy(idx, src, dev):
        return remote(part.at[src], recv.at[idx], rsend.at[idx], rrecv.at[idx], dev)

    r_copies = [
        reduce_copy(0, 2, y_nbr),
        reduce_copy(1, 3, x_nbr),
        reduce_copy(2, 6, y_nbr),
        reduce_copy(3, 7, x_nbr),
        reduce_copy(4, 4, x_nbr),
        reduce_copy(5, 5, y_nbr),
    ]

    for cp in loads[2:]:
        cp.wait()
    for cp in w_copies:
        cp.wait_recv()
    for cp in loads[:2]:
        cp.wait()
    lax.fori_loop(0, 2, project, 0)
    lax.fori_loop(0, 2, mlp, 0)
    g_copies[0].wait_recv()
    g_copies[4].start()
    g_copies[1].wait_recv()
    g_copies[5].start()
    lax.fori_loop(2, 4, project, 0)
    lax.fori_loop(2, 4, mlp, 0)
    g_copies[2].wait_recv()
    g_copies[3].wait_recv()
    lax.fori_loop(4, 6, project, 0)
    lax.fori_loop(0, 6, kv_wait, 0)
    early = [c for c in range(CHUNKS) if c % UNITS < 6]
    late = [c for c in range(CHUNKS) if c % UNITS >= 6]
    attend(2, lambda i: 2 + i, early, emit_state, lambda i, unit: None)
    g_copies[4].wait_recv()
    g_copies[5].wait_recv()
    lax.fori_loop(6, 8, project, 0)
    lax.fori_loop(6, 8, kv_wait, 0)

    def after_first(i, unit):
        add_heads(unit)
        for step in (0, 1):
            @pl.when(i == step)
            def _():
                r_copies[step].start()

    attend(2, lambda i: 2 + i, late, emit_merged, after_first)
    lax.fori_loop(4, 8, mlp, 0)

    def later_unit(i):
        p = i // 2
        return 2 * (3 - p - p // 2) + lax.rem(i, 2)

    def after_later(i, unit):
        add_heads(unit)
        for step in range(4):
            @pl.when(i == step)
            def _():
                if step >= 2:
                    r_copies[step].wait_recv()
                    part[step + 2] += recv[step]
                r_copies[step + 2].start()

    attend(6, later_unit, list(range(CHUNKS)), emit_out, after_later)

    for half, first, second in ((0, 0, 4), (1, 1, 5)):
        r_copies[first].wait_recv()
        r_copies[second].wait_recv()
        span = pl.ds(half * ROWS, ROWS)
        y_ref[span, :] = (xg[half].astype(F32) + part[half] + recv[first] + recv[second]).astype(BF16)
    for cp in g_copies + w_copies + r_copies:
        cp.wait_send()


def solution(mesh):
    def local_block(x_loc, ln_gamma, w_qkv, w_out, w_up, w_down):
        model_dim = x_loc.shape[1]
        head_dim = w_qkv.shape[2] // 3
        ff = w_up.shape[1]
        head_rows = -(-head_dim // 16) * 16
        hbm = pl.BlockSpec(memory_space=pltpu.HBM)
        vmem = pl.BlockSpec(memory_space=pltpu.VMEM)
        dma = pltpu.SemaphoreType.DMA
        return pl.pallas_call(
            functools.partial(block_kernel, head_dim, head_rows),
            out_shape=jax.ShapeDtypeStruct(x_loc.shape, BF16),
            in_specs=[hbm, vmem, hbm, hbm, hbm, hbm],
            out_specs=vmem,
            scratch_shapes=[
                pltpu.VMEM((UNITS, ROWS, model_dim), BF16),
                pltpu.VMEM((UNITS, ROWS, model_dim), BF16),
                pltpu.VMEM((2, HEADS, head_rows, model_dim), BF16),
                pltpu.VMEM((HEADS, LANES, model_dim), BF16),
                pltpu.VMEM((HEADS, head_rows, model_dim), BF16),
                pltpu.VMEM((2, ff, model_dim), BF16),
                pltpu.VMEM((2, ff, model_dim), BF16),
                pltpu.VMEM((UNITS, HEADS, LANES, ROWS), BF16),
                pltpu.VMEM((CHUNKS, HEADS, ROWS, LANES), BF16),
                pltpu.VMEM((CHUNKS, HEADS, head_rows, ROWS), BF16),
                pltpu.VMEM((UNITS, ROWS, model_dim), F32),
                pltpu.VMEM((6, ROWS, model_dim), F32),
                pltpu.VMEM((CHUNKS * ROWS, ROWS), F32),
                pltpu.VMEM((CHUNKS * ROWS, ROWS), F32),
                pltpu.VMEM((8, ROWS), F32),
                pltpu.VMEM((8, ROWS), F32),
                pltpu.VMEM((HEADS, head_rows, ROWS), BF16),
                pltpu.VMEM((2, HEADS, head_rows, ROWS), F32),
                pltpu.VMEM((2, HEADS, 8, ROWS), F32),
                pltpu.VMEM((2, HEADS, 8, ROWS), F32),
                dma((12,)), dma((10,)), dma((10,)), dma((6,)), dma((6,)),
                dma((2, UNITS)), dma((2, UNITS)), dma((6,)), dma((6,)),
            ],
            compiler_params=pltpu.CompilerParams(collective_id=0, has_side_effects=True, vmem_limit_bytes=67043328),
            name="parallel_block",
        )(x_loc, ln_gamma.reshape(1, model_dim), w_qkv.transpose(1, 2, 0), w_out, w_up.T, w_down)

    row_spec = P(("data", "tp"), None)
    return jax.shard_map(local_block, mesh=mesh, in_specs=(row_spec, P(None), P(None, "tp", None), P("tp", None, None), P(None, "tp"), P("tp", None)), out_specs=row_spec, check_vma=False)
```

```python
import functools
import math
import jax
import jax.numpy as jnp
from jax import lax
from jax.experimental import pallas as pl
from jax.experimental.pallas import tpu as pltpu
from jax.sharding import PartitionSpec as P

LN_EPS = 1e-6
LANES = 128
ROWS = 256
UNITS = 8
CHUNKS = 2 * UNITS
HEADS = 4
SUBS = 4
SUB_ROWS = ROWS // SUBS
F32 = jnp.float32
BF16 = jnp.bfloat16
ROW_MAJOR = (((1,), (0,)), ((), ()))
BY_ROWS = (((1,), (1,)), ((), ()))
BY_COLS = (((0,), (0,)), ((), ()))


def dot(a, b, dims=ROW_MAJOR):
    return lax.dot_general(a, b, dims, preferred_element_type=F32)


def gelu_tanh(v):
    return jax.nn.gelu(v, approximate=True)


def block_kernel(head_dim, head_rows, x_hbm, gamma_ref, wqkv_hbm, wout_hbm, w1_hbm, w2_hbm, y_ref,
                 xg, xn, wqv, wk, wout, w1, w2, q_all, k_all, v_all, part, recv, s_even, s_odd, m_even, m_odd, o_t,
                 acc_st, m_st, l_st,
                 load_sem, wsend, wrecv, gsend, grecv, kvsend, kvrecv, rsend, rrecv):
    me = lax.axis_index("tp")
    core = lax.rem(me, 2)
    chip_x = lax.rem(me // 2, 2)
    chip_y = me // 4
    sib = me + 1 - 2 * core
    x_nbr = me + 2 - 4 * chip_x
    y_nbr = me + 4 - 8 * chip_y
    mesh_id = pl.DeviceIdType.MESH

    def remote(src, dst, send, rcv, dev):
        return pltpu.make_async_remote_copy(src_ref=src, dst_ref=dst, send_sem=send, recv_sem=rcv,
                                            device_id={"tp": dev}, device_id_type=mesh_id)

    loads = [pltpu.make_async_copy(x_hbm.at[pl.ds(half * ROWS, ROWS)], xg.at[half], load_sem.at[half]) for half in (0, 1)]
    for cp in loads:
        cp.start()
    barrier = pltpu.get_barrier_semaphore()

    def greet(dev):
        pl.semaphore_signal(barrier, inc=1, device_id={"tp": dev}, device_id_type=mesh_id)

    greet(x_nbr)
    greet(y_nbr)
    wqv[:, :, head_rows - 16:, :] = jnp.zeros((2, HEADS, 16, wqv.shape[3]), BF16)
    wk[:, LANES - 64:, :] = jnp.zeros((HEADS, 64, wk.shape[2]), BF16)
    wout[:, head_rows - 16:, :] = jnp.zeros((HEADS, 16, wout.shape[2]), BF16)
    greet(sib)

    pairs = []
    for hh in (0, 1):
        h = 2 * core + hh
        real = pl.ds(0, head_dim)
        pairs += [
            (wqkv_hbm.at[hh, pl.ds(0, head_dim)], wqv.at[0, h, real]),
            (wqkv_hbm.at[hh, pl.ds(head_dim, head_dim)], wk.at[h, real]),
            (wqkv_hbm.at[hh, pl.ds(2 * head_dim, head_dim)], wqv.at[1, h, real]),
            (wout_hbm.at[hh], wout.at[h, real]),
        ]
    pairs += [(w1_hbm, w1.at[core]), (w2_hbm, w2.at[core])]

    pl.semaphore_wait(barrier, 3)
    for cp in loads:
        cp.wait()

    def gather_copy(src, dst, idx, dev):
        return remote(src, xg.at[dst], gsend.at[idx], grecv.at[idx], dev)

    g_copies = [
        gather_copy(xg.at[0], 2, 0, y_nbr),
        gather_copy(xg.at[1], 3, 1, x_nbr),
        gather_copy(xg.at[0], 4, 2, x_nbr),
        gather_copy(xg.at[1], 5, 3, y_nbr),
        gather_copy(xg.at[2], 6, 4, x_nbr),
        gather_copy(xg.at[3], 7, 5, y_nbr),
    ]
    for cp in g_copies[:4]:
        cp.start()
    w_copies = [remote(src, dst, wsend.at[n], wrecv.at[n], sib) for n, (src, dst) in enumerate(pairs)]
    w_loads = [pltpu.make_async_copy(src, dst, load_sem.at[2 + n]) for n, (src, dst) in enumerate(pairs)]
    for cp in w_copies + w_loads:
        cp.start()

    zero_rows = LANES - head_rows

    def clear(unit, _):
        q_all[unit, :, head_rows:, :] = jnp.zeros((HEADS, zero_rows, ROWS), BF16)
        return 0

    lax.fori_loop(0, UNITS, clear, 0)

    def kv_copies(unit):
        return (
            remote(k_all.at[unit], k_all.at[UNITS + unit], kvsend.at[0, unit], kvrecv.at[0, unit], sib),
            remote(v_all.at[unit], v_all.at[UNITS + unit], kvsend.at[1, unit], kvrecv.at[1, unit], sib),
        )

    def project(unit, _):
        rows = xg[unit].astype(F32)
        mean = jnp.mean(rows, axis=-1, keepdims=True)
        cent = rows - mean
        var = jnp.mean(cent * cent, axis=-1, keepdims=True)
        normed = (cent * lax.rsqrt(var + LN_EPS) * gamma_ref[...][None, :]).astype(BF16)
        xn[unit] = normed
        keys = dot(normed, wk[...].reshape(HEADS * LANES, -1), BY_ROWS)
        qv = dot(wqv[...].reshape(2 * HEADS * head_rows, -1), normed, BY_ROWS).astype(BF16)
        for h in range(HEADS):
            k_all[unit, h] = keys[:, h * LANES:(h + 1) * LANES].astype(BF16)
            q_all[unit, h, :head_rows] = qv[h * head_rows:(h + 1) * head_rows]
            v_all[unit, h] = qv[(HEADS + h) * head_rows:(HEADS + h + 1) * head_rows]
        for cp in kv_copies(unit):
            cp.start()
        return 0

    def mlp(unit, _):
        rows = xn[unit]
        total = None
        for s in (0, 1):
            hidden = gelu_tanh(dot(rows, w1[s], BY_ROWS)).astype(BF16)
            term = dot(hidden, w2[s])
            total = term if total is None else total + term
        part[unit] = total
        return 0

    def kv_wait(unit, _):
        for cp in kv_copies(unit):
            cp.wait()
        return 0

    exp_scale = (head_dim ** -0.5) * math.log2(math.e)
    groups = ROWS // 8
    early = [c for c in range(CHUNKS) if c % UNITS < 6]
    late = [c for c in range(CHUNKS) if c % UNITS >= 6]

    def score_chunk(n, c, h, q, s_ref):
        s = dot(k_all[c, h], q)
        s_ref[pl.ds(n * ROWS, ROWS), :] = s
        return jnp.max(s.reshape(groups, 8, ROWS), axis=0)

    def finish(chunks, h, s_ref, m_ref, unit_n, h_n, s_next, m_next):
        q_n = q_all[unit_n, h_n]
        m = jnp.max(m_ref[...], axis=0, keepdims=True)
        acc = None
        total = None
        m_n = None
        for n, c in enumerate(chunks):
            mc = score_chunk(n, c, h_n, q_n, s_next)
            m_n = mc if m_n is None else jnp.maximum(m_n, mc)
            e = jnp.exp2((s_ref[pl.ds(n * ROWS, ROWS), :] - m) * exp_scale)
            tc = jnp.sum(e.reshape(groups, 8, ROWS), axis=0)
            total = tc if total is None else total + tc
            pv = dot(v_all[c, h], e.astype(BF16))
            acc = pv if acc is None else acc + pv
        m_next[...] = m_n
        return m, jnp.sum(total, axis=0, keepdims=True), acc

    def attend(count, unit_of, chunks, emit, after):
        q = q_all[unit_of(0), 0]
        m = None
        for n, c in enumerate(chunks):
            mc = score_chunk(n, c, 0, q, s_even)
            m = mc if m is None else jnp.maximum(m, mc)
        m_even[...] = m

        def one(i, _):
            unit = unit_of(i)
            unit_next = unit_of(lax.rem(i + 1, count))

            def pair(p, _):
                emit(i, 2 * p, *finish(chunks, 2 * p, s_even, m_even, unit, 2 * p + 1, s_odd, m_odd))
                follow = unit + p * (unit_next - unit)
                emit(i, 2 * p + 1, *finish(chunks, 2 * p + 1, s_odd, m_odd, follow, 2 - 2 * p, s_even, m_even))
                return 0

            lax.fori_loop(0, 2, pair, 0)
            after(i, unit)
            return 0

        lax.fori_loop(0, count, one, 0)

    def emit_state(i, h, m, total, acc):
        m_st[i, h] = jnp.broadcast_to(m, m_st.shape[2:])
        l_st[i, h] = jnp.broadcast_to(total, l_st.shape[2:])
        acc_st[i, h] = acc

    def late_span(n, h):
        return pl.ds((h * len(late) + n) * ROWS, ROWS)

    def late_scores(unit, chunks, start, s_ref):
        for h in range(HEADS):
            q = q_all[unit, h]
            for n, c in enumerate(chunks):
                s_ref[late_span(start + n, h), :] = dot(k_all[c, h], q)

    def late_finish(i, s_ref):
        for h in range(HEADS):
            m = None
            for n in range(len(late)):
                mc = jnp.max(s_ref[late_span(n, h), :].reshape(groups, 8, ROWS), axis=0)
                m = mc if m is None else jnp.maximum(m, mc)
            m = jnp.max(m, axis=0, keepdims=True)
            total = None
            acc = None
            for n, c in enumerate(late):
                e = jnp.exp2((s_ref[late_span(n, h), :] - m) * exp_scale)
                tc = jnp.sum(e.reshape(groups, 8, ROWS), axis=0)
                total = tc if total is None else total + tc
                pv = dot(v_all[c, h], e.astype(BF16))
                acc = pv if acc is None else acc + pv
            emit_merged(i, h, m, jnp.sum(total, axis=0, keepdims=True), acc)

    def emit_merged(i, h, m, total, acc):
        m_old = m_st[i, h][:1]
        top = jnp.maximum(m, m_old)
        a_new = jnp.exp2((m - top) * exp_scale)
        a_old = jnp.exp2((m_old - top) * exp_scale)
        denom = total * a_new + l_st[i, h][:1] * a_old
        o_t[h] = ((acc * a_new + acc_st[i, h] * a_old) / denom).astype(BF16)

    def emit_out(i, h, m, total, acc):
        o_t[h] = (acc / total).astype(BF16)

    def add_heads(unit):
        part[unit] += dot(o_t[...].reshape(HEADS * head_rows, ROWS), wout[...].reshape(HEADS * head_rows, -1), BY_COLS)

    def reduce_copy(idx, src, dev):
        return remote(part.at[src], recv.at[idx], rsend.at[idx], rrecv.at[idx], dev)

    def sub_copies(idx, src, dev):
        copies = []
        for sub in range(SUBS):
            span = pl.ds(sub * SUB_ROWS, SUB_ROWS)
            sem = 2 + (idx - 2) * SUBS + sub
            copies.append(remote(part.at[src, span], recv.at[idx, span], rsend.at[sem], rrecv.at[sem], dev))
        return copies

    r_first = [reduce_copy(0, 2, y_nbr), reduce_copy(1, 3, x_nbr)]
    r_join = [sub_copies(2, 6, y_nbr), sub_copies(3, 7, x_nbr)]
    r_last = [sub_copies(4, 4, x_nbr), sub_copies(5, 5, y_nbr)]

    for cp in w_loads:
        cp.wait()
    for cp in w_copies:
        cp.wait_recv()
    lax.fori_loop(0, 2, project, 0)
    lax.fori_loop(0, 2, mlp, 0)
    g_copies[0].wait_recv()
    g_copies[4].start()
    g_copies[1].wait_recv()
    g_copies[5].start()
    lax.fori_loop(2, 4, project, 0)
    lax.fori_loop(2, 4, mlp, 0)
    g_copies[2].wait_recv()
    g_copies[3].wait_recv()
    lax.fori_loop(4, 6, project, 0)
    lax.fori_loop(0, 6, kv_wait, 0)
    attend(2, lambda i: 2 + i, early, emit_state, lambda i, unit: None)
    g_copies[4].wait_recv()
    g_copies[5].wait_recv()
    lax.fori_loop(6, 8, project, 0)
    late_own = late[:len(late) // 2]
    late_sib = late[len(late) // 2:]
    late_scores(2, late_own, 0, s_even)
    late_scores(3, late_own, 0, s_odd)
    lax.fori_loop(6, 8, kv_wait, 0)
    late_scores(2, late_sib, len(late_own), s_even)
    late_scores(3, late_sib, len(late_own), s_odd)
    late_finish(0, s_even)
    add_heads(2)
    r_first[0].start()
    late_finish(1, s_odd)
    add_heads(3)
    r_first[1].start()
    lax.fori_loop(4, 8, mlp, 0)

    def later_unit(i):
        p = i // 2
        return 2 * (3 - p - p // 2) + lax.rem(i, 2)

    def after_later(i, unit):
        add_heads(unit)
        for step in (0, 1):
            @pl.when(i == step)
            def _():
                for cp in r_join[step]:
                    cp.start()

    attend(6, later_unit, list(range(CHUNKS)), emit_out, after_later)

    for sub in range(SUBS):
        span = pl.ds(sub * SUB_ROWS, SUB_ROWS)
        for n in (0, 1):
            r_join[n][sub].wait_recv()
            part[4 + n, span, :] += recv[2 + n, span, :]
            r_last[n][sub].start()
    for cp in r_first:
        cp.wait_recv()
    for half in (0, 1):
        part[half] += xg[half].astype(F32) + recv[half]
    for sub in range(SUBS):
        span = pl.ds(sub * SUB_ROWS, SUB_ROWS)
        for half in (0, 1):
            r_last[half][sub].wait_recv()
            y_ref[pl.ds(half * ROWS + sub * SUB_ROWS, SUB_ROWS), :] = (part[half, span, :] + recv[4 + half, span, :]).astype(BF16)
    for cp in g_copies + w_copies + r_first:
        cp.wait_send()
    for group in r_join + r_last:
        for cp in group:
            cp.wait_send()


def solution(mesh):
    def local_block(x_loc, ln_gamma, w_qkv, w_out, w_up, w_down):
        model_dim = x_loc.shape[1]
        head_dim = w_qkv.shape[2] // 3
        ff = w_up.shape[1]
        head_rows = -(-head_dim // 16) * 16
        hbm = pl.BlockSpec(memory_space=pltpu.HBM)
        vmem = pl.BlockSpec(memory_space=pltpu.VMEM)
        dma = pltpu.SemaphoreType.DMA
        return pl.pallas_call(
            functools.partial(block_kernel, head_dim, head_rows),
            out_shape=pltpu.VMEM(x_loc.shape, BF16),
            in_specs=[hbm, vmem, hbm, hbm, hbm, hbm],
            out_specs=vmem,
            scratch_shapes=[
                pltpu.VMEM((UNITS, ROWS, model_dim), BF16),
                pltpu.VMEM((UNITS, ROWS, model_dim), BF16),
                pltpu.VMEM((2, HEADS, head_rows, model_dim), BF16),
                pltpu.VMEM((HEADS, LANES, model_dim), BF16),
                pltpu.VMEM((HEADS, head_rows, model_dim), BF16),
                pltpu.VMEM((2, ff, model_dim), BF16),
                pltpu.VMEM((2, ff, model_dim), BF16),
                pltpu.VMEM((UNITS, HEADS, LANES, ROWS), BF16),
                pltpu.VMEM((CHUNKS, HEADS, ROWS, LANES), BF16),
                pltpu.VMEM((CHUNKS, HEADS, head_rows, ROWS), BF16),
                pltpu.VMEM((UNITS, ROWS, model_dim), F32),
                pltpu.VMEM((6, ROWS, model_dim), F32),
                pltpu.VMEM((CHUNKS * ROWS, ROWS), F32),
                pltpu.VMEM((CHUNKS * ROWS, ROWS), F32),
                pltpu.VMEM((8, ROWS), F32),
                pltpu.VMEM((8, ROWS), F32),
                pltpu.VMEM((HEADS, head_rows, ROWS), BF16),
                pltpu.VMEM((2, HEADS, head_rows, ROWS), F32),
                pltpu.VMEM((2, HEADS, 8, ROWS), F32),
                pltpu.VMEM((2, HEADS, 8, ROWS), F32),
                dma((12,)), dma((10,)), dma((10,)), dma((6,)), dma((6,)),
                dma((2, UNITS)), dma((2, UNITS)), dma((2 + 4 * SUBS,)), dma((2 + 4 * SUBS,)),
            ],
            compiler_params=pltpu.CompilerParams(collective_id=0, has_side_effects=True, vmem_limit_bytes=64000000),
            name="parallel_block",
        )(x_loc, ln_gamma, w_qkv.transpose(1, 2, 0), w_out, w_up.T, w_down)

    row_spec = P(("data", "tp"), None)
    return jax.shard_map(local_block, mesh=mesh, in_specs=(row_spec, P(None), P(None, "tp", None), P("tp", None, None), P(None, "tp"), P("tp", None)), out_specs=row_spec, check_vma=False)
```

```python
import functools
import math
import jax
import jax.numpy as jnp
from jax import lax
from jax.experimental import pallas as pl
from jax.experimental.pallas import tpu as pltpu
from jax.sharding import PartitionSpec as P

LN_EPS = 1e-6
LANES = 128
ROWS = 256
UNITS = 8
CHUNKS = 2 * UNITS
HEADS = 4
HALF = ROWS // 2
QUARTER = ROWS // 4
F32 = jnp.float32
BF16 = jnp.bfloat16
ROW_MAJOR = (((1,), (0,)), ((), ()))
BY_ROWS = (((1,), (1,)), ((), ()))
BY_COLS = (((0,), (0,)), ((), ()))


def dot(a, b, dims=ROW_MAJOR):
    return lax.dot_general(a, b, dims, preferred_element_type=F32)


def gelu_tanh(v):
    return jax.nn.gelu(v, approximate=True)


def block_kernel(head_dim, head_rows, x_hbm, gamma_ref, wqkv_hbm, wout_hbm, w1_hbm, w2_hbm, y_ref,
                 xg, xn, wqv, wk, wout, w1, w2, q_all, k_all, v_all, part, recv, s_even, s_odd, m_even, m_odd, o_t,
                 acc_st, m_st, l_st, m_all,
                 load_sem, wsend, wrecv, gsend, grecv, kvsend, kvrecv, rsend, rrecv):
    me = lax.axis_index("tp")
    core = lax.rem(me, 2)
    chip_x = lax.rem(me // 2, 2)
    chip_y = me // 4
    sib = me + 1 - 2 * core
    x_nbr = me + 2 - 4 * chip_x
    y_nbr = me + 4 - 8 * chip_y
    mesh_id = pl.DeviceIdType.MESH

    def remote(src, dst, send, rcv, dev):
        return pltpu.make_async_remote_copy(src_ref=src, dst_ref=dst, send_sem=send, recv_sem=rcv,
                                            device_id={"tp": dev}, device_id_type=mesh_id)

    loads = [pltpu.make_async_copy(x_hbm.at[pl.ds(half * ROWS, ROWS)], xg.at[half], load_sem.at[half]) for half in (0, 1)]
    for cp in loads:
        cp.start()
    barrier = pltpu.get_barrier_semaphore()

    def greet(dev):
        pl.semaphore_signal(barrier, inc=1, device_id={"tp": dev}, device_id_type=mesh_id)

    greet(x_nbr)
    greet(y_nbr)
    wqv[:, :, head_rows - 16:, :] = jnp.zeros((2, HEADS, 16, wqv.shape[3]), BF16)
    wk[:, LANES - 64:, :] = jnp.zeros((HEADS, 64, wk.shape[2]), BF16)
    wout[:, head_rows - 16:, :] = jnp.zeros((HEADS, 16, wout.shape[2]), BF16)
    greet(sib)

    pairs = []
    for hh in (0, 1):
        h = 2 * core + hh
        real = pl.ds(0, head_dim)
        pairs += [
            (wqkv_hbm.at[hh, pl.ds(0, head_dim)], wqv.at[0, h, real]),
            (wqkv_hbm.at[hh, pl.ds(head_dim, head_dim)], wk.at[h, real]),
            (wqkv_hbm.at[hh, pl.ds(2 * head_dim, head_dim)], wqv.at[1, h, real]),
            (wout_hbm.at[hh], wout.at[h, real]),
        ]
    pairs += [(w1_hbm, w1.at[core]), (w2_hbm, w2.at[core])]

    pl.semaphore_wait(barrier, 3)
    for cp in loads:
        cp.wait()

    top, low = pl.ds(0, HALF), pl.ds(HALF, HALF)
    parts = (top, low)

    def gather_copy(src, src_span, dst, dst_span, idx, dev):
        return remote(xg.at[src, src_span], xg.at[dst, dst_span], gsend.at[idx], grecv.at[idx], dev)

    g_first = [(gather_copy(0, parts[j], 2 + j, top, j, y_nbr), gather_copy(1, parts[j], 2 + j, low, 2 + j, x_nbr)) for j in (0, 1)]
    g_second = [(gather_copy(0, parts[j], 4 + j, top, 4 + j, x_nbr), gather_copy(1, parts[j], 4 + j, low, 6 + j, y_nbr)) for j in (0, 1)]
    g_diag = [(gather_copy(2 + j, top, 6 + j, top, 8 + j, x_nbr), gather_copy(2 + j, low, 6 + j, low, 10 + j, y_nbr)) for j in (0, 1)]
    g_copies = [cp for group in (g_first, g_second, g_diag) for two in group for cp in two]
    for cp in g_copies[:8]:
        cp.start()
    w_copies = [remote(src, dst, wsend.at[n], wrecv.at[n], sib) for n, (src, dst) in enumerate(pairs)]
    w_loads = [pltpu.make_async_copy(src, dst, load_sem.at[2 + n]) for n, (src, dst) in enumerate(pairs)]
    for cp in w_copies + w_loads:
        cp.start()

    zero_rows = LANES - head_rows

    def clear(unit, _):
        q_all[unit, :, head_rows:, :] = jnp.zeros((HEADS, zero_rows, ROWS), BF16)
        return 0

    lax.fori_loop(0, UNITS, clear, 0)

    def kv_copies(unit):
        return (
            remote(k_all.at[unit], k_all.at[UNITS + unit], kvsend.at[0, unit], kvrecv.at[0, unit], sib),
            remote(v_all.at[unit], v_all.at[UNITS + unit], kvsend.at[1, unit], kvrecv.at[1, unit], sib),
        )

    def project(unit, _):
        rows = xg[unit].astype(F32)
        mean = jnp.mean(rows, axis=-1, keepdims=True)
        cent = rows - mean
        var = jnp.mean(cent * cent, axis=-1, keepdims=True)
        normed = (cent * lax.rsqrt(var + LN_EPS) * gamma_ref[...][None, :]).astype(BF16)
        xn[unit] = normed
        keys = dot(normed, wk[...].reshape(HEADS * LANES, -1), BY_ROWS)
        for h in range(HEADS):
            k_all[unit, h] = keys[:, h * LANES:(h + 1) * LANES].astype(BF16)
        k_copy, v_copy = kv_copies(unit)
        k_copy.start()
        values = dot(wqv[1].reshape(HEADS * head_rows, -1), normed, BY_ROWS).astype(BF16)
        for h in range(HEADS):
            v_all[unit, h] = values[h * head_rows:(h + 1) * head_rows]
        v_copy.start()
        return 0

    def project_queries(unit, _):
        queries = dot(wqv[0].reshape(HEADS * head_rows, -1), xn[unit], BY_ROWS).astype(BF16)
        for h in range(HEADS):
            q_all[unit, h, :head_rows] = queries[h * head_rows:(h + 1) * head_rows]
        return 0

    def project_both(unit, _):
        project(unit, 0)
        return project_queries(unit, 0)

    def mlp(unit, _):
        rows = xn[unit]
        total = None
        for s in (0, 1):
            hidden = gelu_tanh(dot(rows, w1[s], BY_ROWS)).astype(BF16)
            term = dot(hidden, w2[s])
            total = term if total is None else total + term
        part[unit] = total
        return 0

    def kv_wait(unit, _):
        for cp in kv_copies(unit):
            cp.wait()
        return 0

    exp_scale = (head_dim ** -0.5) * math.log2(math.e)
    groups = ROWS // 8

    def chunks_of(*units):
        return list(units) + [UNITS + u for u in units]


    def score_chunk(n, c, h, q, s_ref):
        s = dot(k_all[c, h], q)
        s_ref[pl.ds(n * ROWS, ROWS), :] = s
        return jnp.max(s.reshape(groups, 8, ROWS), axis=0)

    def finish(chunks, h, s_ref, m_ref, unit_n, h_n, s_next, m_next):
        q_n = q_all[unit_n, h_n]
        m = jnp.max(m_ref[...], axis=0, keepdims=True)
        acc = None
        total = None
        m_n = None
        for n, c in enumerate(chunks):
            mc = score_chunk(n, c, h_n, q_n, s_next)
            m_n = mc if m_n is None else jnp.maximum(m_n, mc)
            e = jnp.exp2((s_ref[pl.ds(n * ROWS, ROWS), :] - m) * exp_scale)
            tc = jnp.sum(e.reshape(groups, 8, ROWS), axis=0)
            total = tc if total is None else total + tc
            pv = dot(v_all[c, h], e.astype(BF16))
            acc = pv if acc is None else acc + pv
        m_next[...] = m_n
        return m, jnp.sum(total, axis=0, keepdims=True), acc

    def attend(count, unit_of, chunks, emit, after):
        q = q_all[unit_of(0), 0]
        m = None
        for n, c in enumerate(chunks):
            mc = score_chunk(n, c, 0, q, s_even)
            m = mc if m is None else jnp.maximum(m, mc)
        m_even[...] = m

        def one(i, _):
            unit = unit_of(i)
            unit_next = unit_of(lax.rem(i + 1, count))

            def pair(p, _):
                emit(i, 2 * p, *finish(chunks, 2 * p, s_even, m_even, unit, 2 * p + 1, s_odd, m_odd))
                follow = unit + p * (unit_next - unit)
                emit(i, 2 * p + 1, *finish(chunks, 2 * p + 1, s_odd, m_odd, follow, 2 - 2 * p, s_even, m_even))
                return 0

            lax.fori_loop(0, 2, pair, 0)
            after(i, unit)
            return 0

        lax.fori_loop(0, count, one, 0)

    def emit_state(i, h, m, total, acc):
        m_st[i, h] = jnp.broadcast_to(m, m_st.shape[2:])
        l_st[i, h] = jnp.broadcast_to(total, l_st.shape[2:])
        acc_st[i, h] = acc

    def more_chunks(i, chunks, emit, s_ref):
        for h in range(HEADS):
            q = q_all[2 + i, h]
            m = None
            for n, c in enumerate(chunks):
                mc = score_chunk(h * len(chunks) + n, c, h, q, s_ref)
                m = mc if m is None else jnp.maximum(m, mc)
            m_all[h] = m
        for h in range(HEADS):
            m = jnp.max(m_all[h], axis=0, keepdims=True)
            total = None
            acc = None
            for n, c in enumerate(chunks):
                e = jnp.exp2((s_ref[pl.ds((h * len(chunks) + n) * ROWS, ROWS), :] - m) * exp_scale)
                tc = jnp.sum(e.reshape(groups, 8, ROWS), axis=0)
                total = tc if total is None else total + tc
                pv = dot(v_all[c, h], e.astype(BF16))
                acc = pv if acc is None else acc + pv
            emit(i, h, m, jnp.sum(total, axis=0, keepdims=True), acc)

    def joined(i, h, m, total, acc):
        m_old = m_st[i, h][:1]
        high = jnp.maximum(m, m_old)
        a_new = jnp.exp2((m - high) * exp_scale)
        a_old = jnp.exp2((m_old - high) * exp_scale)
        return high, total * a_new + l_st[i, h][:1] * a_old, acc * a_new + acc_st[i, h] * a_old

    def emit_joined(i, h, m, total, acc):
        emit_state(i, h, *joined(i, h, m, total, acc))

    def emit_last(i, h, m, total, acc):
        emit_out(i, h, *joined(i, h, m, total, acc))

    def emit_out(i, h, m, total, acc):
        o_t[h] = (acc / total).astype(BF16)

    def add_heads(unit):
        part[unit] += dot(o_t[...].reshape(HEADS * head_rows, ROWS), wout[...].reshape(HEADS * head_rows, -1), BY_COLS)

    def reduce_copy(src, dst, start, size, sem, dev):
        span = pl.ds(start, size)
        return remote(part.at[src, span], recv.at[dst, span], rsend.at[sem], rrecv.at[sem], dev)

    r_first = [(reduce_copy(2 + j, j, 0, HALF, 2 * j, y_nbr), reduce_copy(2 + j, j, HALF, HALF, 2 * j + 1, x_nbr)) for j in (0, 1)]
    quarters = (0, 2, 1, 3)

    def quarter_copies(src, dst, sem, first, second):
        return [reduce_copy(src, dst, n * QUARTER, QUARTER, sem + n, first if n < 2 else second) for n in range(4)]

    r_join = [quarter_copies(6 + j, 2 + j, 4 + 4 * j, y_nbr, x_nbr) for j in (0, 1)]
    r_last = [quarter_copies(4 + j, 4 + j, 12 + 4 * j, x_nbr, y_nbr) for j in (0, 1)]

    for cp in w_loads:
        cp.wait()
    for cp in w_copies:
        cp.wait_recv()
    lax.fori_loop(0, 2, project_both, 0)
    lax.fori_loop(0, 2, mlp, 0)
    for j in (0, 1):
        for cp, onward in zip(g_first[j], g_diag[j]):
            cp.wait_recv()
            onward.start()
    lax.fori_loop(2, 4, project_both, 0)
    lax.fori_loop(2, 4, mlp, 0)
    lax.fori_loop(0, 4, kv_wait, 0)
    attend(2, lambda i: 2 + i, chunks_of(0, 1, 2, 3), emit_state, lambda i, unit: None)
    for j in (0, 1):
        for cp in g_second[j]:
            cp.wait_recv()
    lax.fori_loop(4, 6, project_both, 0)
    lax.fori_loop(4, 6, kv_wait, 0)

    def next_chunks(i, _):
        more_chunks(i, chunks_of(4, 5), emit_joined, s_even)
        return 0

    lax.fori_loop(0, 2, next_chunks, 0)
    for cp in g_diag[0]:
        cp.wait_recv()
    project_both(6, 0)
    kv_wait(6, 0)

    def diag_chunks(i, _):
        more_chunks(i, chunks_of(6), emit_joined, s_even)
        return 0

    lax.fori_loop(0, 2, diag_chunks, 0)
    for cp in g_diag[1]:
        cp.wait_recv()
    project(7, 0)
    project_queries(7, 0)
    kv_wait(7, 0)
    for j in (0, 1):
        more_chunks(j, chunks_of(7), emit_last, s_even)
        add_heads(2 + j)
        for cp in r_first[j]:
            cp.start()
    lax.fori_loop(4, 8, mlp, 0)

    def later_unit(i):
        p = i // 2
        return 2 * (3 - p - p // 2) + lax.rem(i, 2)

    def after_later(i, unit):
        add_heads(unit)
        for step in (0, 1):
            @pl.when(i == step)
            def _():
                for n in quarters:
                    r_join[step][n].start()

    attend(6, later_unit, list(range(CHUNKS)), emit_out, after_later)

    for j in (0, 1):
        for n in quarters:
            span = pl.ds(n * QUARTER, QUARTER)
            r_join[j][n].wait_recv()
            part[4 + j, span, :] += recv[2 + j, span, :]
            r_last[j][n].start()
    for j in (0, 1):
        for half in (0, 1):
            r_first[j][half].wait_recv()
            part[half, parts[j], :] += xg[half, parts[j], :].astype(F32) + recv[j, parts[half], :]
    for j in (0, 1):
        for n in quarters:
            half, start = n // 2, j * HALF + (n % 2) * QUARTER
            r_last[j][n].wait_recv()
            total = part[half, pl.ds(start, QUARTER), :] + recv[4 + j, pl.ds(n * QUARTER, QUARTER), :]
            y_ref[pl.ds(half * ROWS + start, QUARTER), :] = total.astype(BF16)
    for cp in g_copies + w_copies:
        cp.wait_send()
    for group in r_first + r_join + r_last:
        for cp in group:
            cp.wait_send()


def solution(mesh):
    def local_block(x_loc, ln_gamma, w_qkv, w_out, w_up, w_down):
        model_dim = x_loc.shape[1]
        head_dim = w_qkv.shape[2] // 3
        ff = w_up.shape[1]
        head_rows = -(-head_dim // 16) * 16
        hbm = pl.BlockSpec(memory_space=pltpu.HBM)
        vmem = pl.BlockSpec(memory_space=pltpu.VMEM)
        dma = pltpu.SemaphoreType.DMA
        return pl.pallas_call(
            functools.partial(block_kernel, head_dim, head_rows),
            out_shape=pltpu.VMEM(x_loc.shape, BF16),
            in_specs=[hbm, vmem, hbm, hbm, hbm, hbm],
            out_specs=vmem,
            scratch_shapes=[
                pltpu.VMEM((UNITS, ROWS, model_dim), BF16),
                pltpu.VMEM((UNITS, ROWS, model_dim), BF16),
                pltpu.VMEM((2, HEADS, head_rows, model_dim), BF16),
                pltpu.VMEM((HEADS, LANES, model_dim), BF16),
                pltpu.VMEM((HEADS, head_rows, model_dim), BF16),
                pltpu.VMEM((2, ff, model_dim), BF16),
                pltpu.VMEM((2, ff, model_dim), BF16),
                pltpu.VMEM((UNITS, HEADS, LANES, ROWS), BF16),
                pltpu.VMEM((CHUNKS, HEADS, ROWS, LANES), BF16),
                pltpu.VMEM((CHUNKS, HEADS, head_rows, ROWS), BF16),
                pltpu.VMEM((UNITS, ROWS, model_dim), F32),
                pltpu.VMEM((6, ROWS, model_dim), F32),
                pltpu.VMEM((CHUNKS * ROWS, ROWS), F32),
                pltpu.VMEM((CHUNKS * ROWS, ROWS), F32),
                pltpu.VMEM((8, ROWS), F32),
                pltpu.VMEM((8, ROWS), F32),
                pltpu.VMEM((HEADS, head_rows, ROWS), BF16),
                pltpu.VMEM((2, HEADS, head_rows, ROWS), F32),
                pltpu.VMEM((2, HEADS, 8, ROWS), F32),
                pltpu.VMEM((2, HEADS, 8, ROWS), F32),
                pltpu.VMEM((HEADS, 8, ROWS), F32),
                dma((12,)), dma((10,)), dma((10,)), dma((12,)), dma((12,)),
                dma((2, UNITS)), dma((2, UNITS)), dma((20,)), dma((20,)),
            ],
            compiler_params=pltpu.CompilerParams(collective_id=0, has_side_effects=True, vmem_limit_bytes=64000000),
            name="parallel_block",
        )(x_loc, ln_gamma, w_qkv.transpose(1, 2, 0), w_out, w_up.T, w_down)

    row_spec = P(("data", "tp"), None)
    return jax.shard_map(local_block, mesh=mesh, in_specs=(row_spec, P(None), P(None, "tp", None), P("tp", None, None), P(None, "tp"), P("tp", None)), out_specs=row_spec, check_vma=False)
```

```python
import functools
import math
import jax
import jax.numpy as jnp
from jax import lax
from jax.experimental import pallas as pl
from jax.experimental.pallas import tpu as pltpu
from jax.sharding import PartitionSpec as P

LN_EPS = 1e-6
LANES = 128
ROWS = 256
UNITS = 8
CHUNKS = 2 * UNITS
HEADS = 4
HALF = ROWS // 2
QUARTER = ROWS // 4
F32 = jnp.float32
BF16 = jnp.bfloat16
ROW_MAJOR = (((1,), (0,)), ((), ()))
BY_ROWS = (((1,), (1,)), ((), ()))
BY_COLS = (((0,), (0,)), ((), ()))


def dot(a, b, dims=ROW_MAJOR):
    return lax.dot_general(a, b, dims, preferred_element_type=F32)


def gelu_tanh(v):
    return jax.nn.gelu(v, approximate=True)


def block_kernel(head_dim, head_rows, x_hbm, gamma_ref, wqkv_hbm, wout_hbm, w1_hbm, w2_hbm, y_ref,
                 xg, xn, wqv, wk, wout, w1, w2, q_all, k_all, v_all, part, recv, s_even, s_odd, m_even, m_odd, o_t,
                 acc_st, m_st, l_st, m_all,
                 load_sem, wsend, wrecv, gsend, grecv, kvsend, kvrecv, rsend, rrecv):
    me = lax.axis_index("tp")
    core = lax.rem(me, 2)
    chip_x = lax.rem(me // 2, 2)
    chip_y = me // 4
    sib = me + 1 - 2 * core
    x_nbr = me + 2 - 4 * chip_x
    y_nbr = me + 4 - 8 * chip_y
    mesh_id = pl.DeviceIdType.MESH

    def remote(src, dst, send, rcv, dev):
        return pltpu.make_async_remote_copy(src_ref=src, dst_ref=dst, send_sem=send, recv_sem=rcv,
                                            device_id={"tp": dev}, device_id_type=mesh_id)

    loads = [pltpu.make_async_copy(x_hbm.at[pl.ds(half * ROWS, ROWS)], xg.at[half], load_sem.at[half]) for half in (0, 1)]
    for cp in loads:
        cp.start()
    barrier = pltpu.get_barrier_semaphore()

    def greet(dev):
        pl.semaphore_signal(barrier, inc=1, device_id={"tp": dev}, device_id_type=mesh_id)

    greet(x_nbr)
    greet(y_nbr)
    wqv[:, :, head_rows - 16:, :] = jnp.zeros((2, HEADS, 16, wqv.shape[3]), BF16)
    wk[:, LANES - 64:, :] = jnp.zeros((HEADS, 64, wk.shape[2]), BF16)
    wout[:, head_rows - 16:, :] = jnp.zeros((HEADS, 16, wout.shape[2]), BF16)
    greet(sib)

    pairs = []
    for hh in (0, 1):
        h = 2 * core + hh
        real = pl.ds(0, head_dim)
        pairs += [
            (wqkv_hbm.at[hh, pl.ds(0, head_dim)], wqv.at[0, h, real]),
            (wqkv_hbm.at[hh, pl.ds(head_dim, head_dim)], wk.at[h, real]),
            (wqkv_hbm.at[hh, pl.ds(2 * head_dim, head_dim)], wqv.at[1, h, real]),
            (wout_hbm.at[hh], wout.at[h, real]),
        ]
    pairs += [(w1_hbm, w1.at[core]), (w2_hbm, w2.at[core])]

    pl.semaphore_wait(barrier, 3)
    for cp in loads:
        cp.wait()

    top, low = pl.ds(0, HALF), pl.ds(HALF, HALF)
    parts = (top, low)

    def gather_copy(src, src_span, dst, dst_span, idx, dev):
        return remote(xg.at[src, src_span], xg.at[dst, dst_span], gsend.at[idx], grecv.at[idx], dev)

    g_first = [(gather_copy(0, parts[j], 2 + j, top, j, y_nbr), gather_copy(1, parts[j], 2 + j, low, 2 + j, x_nbr)) for j in (0, 1)]
    g_second = [(gather_copy(0, parts[j], 4 + j, top, 4 + j, x_nbr), gather_copy(1, parts[j], 4 + j, low, 6 + j, y_nbr)) for j in (0, 1)]
    g_diag = [(gather_copy(2, top, 6, top, 8, x_nbr), gather_copy(2, low, 6, low, 9, y_nbr))]
    for q in (0, 1):
        q_top, q_low = pl.ds(q * QUARTER, QUARTER), pl.ds(HALF + q * QUARTER, QUARTER)
        g_diag.append((gather_copy(3, q_top, 7, q_top, 10 + q, x_nbr), gather_copy(3, q_low, 7, q_low, 12 + q, y_nbr)))
    g_copies = [cp for group in (g_first, g_second, g_diag) for two in group for cp in two]
    for cp in g_copies[:8]:
        cp.start()
    w_copies = [remote(src, dst, wsend.at[n], wrecv.at[n], sib) for n, (src, dst) in enumerate(pairs)]
    w_loads = [pltpu.make_async_copy(src, dst, load_sem.at[2 + n]) for n, (src, dst) in enumerate(pairs)]
    for cp in w_copies + w_loads:
        cp.start()

    zero_rows = LANES - head_rows

    def clear(unit, _):
        q_all[unit, :, head_rows:, :] = jnp.zeros((HEADS, zero_rows, ROWS), BF16)
        return 0

    lax.fori_loop(0, UNITS, clear, 0)

    def kv_copies(unit):
        return (
            remote(k_all.at[unit], k_all.at[UNITS + unit], kvsend.at[0, unit], kvrecv.at[0, unit], sib),
            remote(v_all.at[unit], v_all.at[UNITS + unit], kvsend.at[1, unit], kvrecv.at[1, unit], sib),
        )

    def normalize(rows):
        rows = rows.astype(F32)
        mean = jnp.mean(rows, axis=-1, keepdims=True)
        cent = rows - mean
        var = jnp.mean(cent * cent, axis=-1, keepdims=True)
        return (cent * lax.rsqrt(var + LN_EPS) * gamma_ref[...][None, :]).astype(BF16)

    last = UNITS - 1

    def last_copies(q):
        span = parts[q]
        return (
            remote(k_all.at[last, :, span], k_all.at[UNITS + last, :, span], kvsend.at[q, last], kvrecv.at[q, last], sib),
            remote(v_all.at[last, :, :, span], v_all.at[UNITS + last, :, :, span], kvsend.at[q, UNITS], kvrecv.at[q, UNITS], sib),
        )

    def project_last(q):
        spans = (pl.ds(q * QUARTER, QUARTER), pl.ds(HALF + q * QUARTER, QUARTER))
        normed = normalize(jnp.concatenate([xg[last, span] for span in spans], axis=0))
        keys = dot(normed, wk[...].reshape(HEADS * LANES, -1), BY_ROWS)
        for h in range(HEADS):
            k_all[last, h, parts[q]] = keys[:, h * LANES:(h + 1) * LANES].astype(BF16)
        k_copy, v_copy = last_copies(q)
        k_copy.start()
        values = dot(wqv[1].reshape(HEADS * head_rows, -1), normed, BY_ROWS).astype(BF16)
        for h in range(HEADS):
            v_all[last, h, :, parts[q]] = values[h * head_rows:(h + 1) * head_rows]
        v_copy.start()
        for n, span in enumerate(spans):
            xn[last, span] = normed[n * QUARTER:(n + 1) * QUARTER]

    def project(unit, _):
        normed = normalize(xg[unit])
        xn[unit] = normed
        keys = dot(normed, wk[...].reshape(HEADS * LANES, -1), BY_ROWS)
        for h in range(HEADS):
            k_all[unit, h] = keys[:, h * LANES:(h + 1) * LANES].astype(BF16)
        k_copy, v_copy = kv_copies(unit)
        k_copy.start()
        values = dot(wqv[1].reshape(HEADS * head_rows, -1), normed, BY_ROWS).astype(BF16)
        for h in range(HEADS):
            v_all[unit, h] = values[h * head_rows:(h + 1) * head_rows]
        v_copy.start()
        return 0

    def project_queries(unit, _):
        queries = dot(wqv[0].reshape(HEADS * head_rows, -1), xn[unit], BY_ROWS).astype(BF16)
        for h in range(HEADS):
            q_all[unit, h, :head_rows] = queries[h * head_rows:(h + 1) * head_rows]
        return 0

    def project_both(unit, _):
        project(unit, 0)
        return project_queries(unit, 0)

    def mlp(unit, _):
        rows = xn[unit]
        total = None
        for s in (0, 1):
            hidden = gelu_tanh(dot(rows, w1[s], BY_ROWS)).astype(BF16)
            term = dot(hidden, w2[s])
            total = term if total is None else total + term
        part[unit] = total
        return 0

    def kv_wait(unit, _):
        for cp in kv_copies(unit):
            cp.wait()
        return 0

    exp_scale = (head_dim ** -0.5) * math.log2(math.e)
    groups = ROWS // 8

    def chunks_of(*units):
        return list(units) + [UNITS + u for u in units]


    def score_chunk(n, c, h, q, s_ref):
        s = dot(k_all[c, h], q)
        s_ref[pl.ds(n * ROWS, ROWS), :] = s
        return jnp.max(s.reshape(groups, 8, ROWS), axis=0)

    def finish(chunks, h, s_ref, m_ref, unit_n, h_n, s_next, m_next):
        q_n = q_all[unit_n, h_n]
        m = jnp.max(m_ref[...], axis=0, keepdims=True)
        acc = None
        total = None
        m_n = None
        for n, c in enumerate(chunks):
            mc = score_chunk(n, c, h_n, q_n, s_next)
            m_n = mc if m_n is None else jnp.maximum(m_n, mc)
            e = jnp.exp2((s_ref[pl.ds(n * ROWS, ROWS), :] - m) * exp_scale)
            tc = jnp.sum(e.reshape(groups, 8, ROWS), axis=0)
            total = tc if total is None else total + tc
            pv = dot(v_all[c, h], e.astype(BF16))
            acc = pv if acc is None else acc + pv
        m_next[...] = m_n
        return m, jnp.sum(total, axis=0, keepdims=True), acc

    def attend(count, unit_of, chunks, emit, after):
        q = q_all[unit_of(0), 0]
        m = None
        for n, c in enumerate(chunks):
            mc = score_chunk(n, c, 0, q, s_even)
            m = mc if m is None else jnp.maximum(m, mc)
        m_even[...] = m

        def one(i, _):
            unit = unit_of(i)
            unit_next = unit_of(lax.rem(i + 1, count))

            def pair(p, _):
                emit(i, 2 * p, *finish(chunks, 2 * p, s_even, m_even, unit, 2 * p + 1, s_odd, m_odd))
                follow = unit + p * (unit_next - unit)
                emit(i, 2 * p + 1, *finish(chunks, 2 * p + 1, s_odd, m_odd, follow, 2 - 2 * p, s_even, m_even))
                return 0

            lax.fori_loop(0, 2, pair, 0)
            after(i, unit)
            return 0

        lax.fori_loop(0, count, one, 0)

    def emit_state(i, h, m, total, acc):
        m_st[h] = jnp.broadcast_to(m, m_st.shape[1:])
        l_st[h] = jnp.broadcast_to(total, l_st.shape[1:])
        acc_st[h] = acc

    def more_chunks(pieces, emit, s_ref, before_values=None):
        size = ROWS if pieces[0][1] is None else HALF

        def rows_of(h, n):
            return pl.ds((h * len(pieces) + n) * size, size)

        for h in range(HEADS):
            q = q_all[2, h]
            m = None
            for n, (c, part_no) in enumerate(pieces):
                s = dot(k_all[c, h] if part_no is None else k_all[c, h, parts[part_no]], q)
                s_ref[rows_of(h, n), :] = s
                mc = jnp.max(s.reshape(size // 8, 8, ROWS), axis=0)
                m = mc if m is None else jnp.maximum(m, mc)
            m_all[h] = m
        if before_values is not None:
            before_values()
        for h in range(HEADS):
            m = jnp.max(m_all[h], axis=0, keepdims=True)
            total = None
            acc = None
            for n, (c, part_no) in enumerate(pieces):
                e = jnp.exp2((s_ref[rows_of(h, n), :] - m) * exp_scale)
                tc = jnp.sum(e.reshape(size // 8, 8, ROWS), axis=0)
                total = tc if total is None else total + tc
                v = v_all[c, h] if part_no is None else v_all[c, h, :, parts[part_no]]
                pv = dot(v, e.astype(BF16))
                acc = pv if acc is None else acc + pv
            emit(0, h, m, jnp.sum(total, axis=0, keepdims=True), acc)

    def joined(h, m, total, acc):
        m_old = m_st[h][:1]
        high = jnp.maximum(m, m_old)
        a_new = jnp.exp2((m - high) * exp_scale)
        a_old = jnp.exp2((m_old - high) * exp_scale)
        return high, total * a_new + l_st[h][:1] * a_old, acc * a_new + acc_st[h] * a_old

    def emit_joined(i, h, m, total, acc):
        emit_state(i, h, *joined(h, m, total, acc))

    def emit_last(i, h, m, total, acc):
        emit_out(i, h, *joined(h, m, total, acc))

    def emit_out(i, h, m, total, acc):
        o_t[h] = (acc / total).astype(BF16)

    def add_heads(unit):
        part[unit] += dot(o_t[...].reshape(HEADS * head_rows, ROWS), wout[...].reshape(HEADS * head_rows, -1), BY_COLS)

    def reduce_copy(src, dst, start, size, sem, dev):
        span = pl.ds(start, size)
        return remote(part.at[src, span], recv.at[dst, span], rsend.at[sem], rrecv.at[sem], dev)

    r_first = [(reduce_copy(2 + j, j, 0, HALF, 2 * j, y_nbr), reduce_copy(2 + j, j, HALF, HALF, 2 * j + 1, x_nbr)) for j in (0, 1)]
    quarters = (0, 2, 1, 3)

    def quarter_copies(src, dst, sem, first, second):
        return [reduce_copy(src, dst, n * QUARTER, QUARTER, sem + n, first if n < 2 else second) for n in range(4)]

    r_join = [quarter_copies(6 + j, 2 + j, 4 + 4 * j, y_nbr, x_nbr) for j in (0, 1)]
    r_last = [quarter_copies(4 + j, 4 + j, 12 + 4 * j, x_nbr, y_nbr) for j in (0, 1)]

    for cp in w_loads:
        cp.wait()
    for cp in w_copies:
        cp.wait_recv()
    lax.fori_loop(0, 2, project_both, 0)
    lax.fori_loop(0, 2, mlp, 0)
    for j in (0, 1):
        for side in (0, 1):
            g_first[j][side].wait_recv()
            for two in g_diag[:1] if j == 0 else g_diag[1:]:
                two[side].start()
    lax.fori_loop(2, 4, project_both, 0)
    lax.fori_loop(0, 4, kv_wait, 0)
    attend(1, lambda i: 2, chunks_of(0, 1, 2, 3), emit_state, lambda i, unit: None)
    lax.fori_loop(2, 4, mlp, 0)
    for j in (0, 1):
        for cp in g_second[j]:
            cp.wait_recv()
    lax.fori_loop(4, 6, project_both, 0)
    lax.fori_loop(4, 6, kv_wait, 0)
    more_chunks([(c, None) for c in chunks_of(4, 5)], emit_joined, s_even)
    for cp in g_diag[0]:
        cp.wait_recv()
    project_both(6, 0)
    kv_wait(6, 0)
    more_chunks([(c, None) for c in chunks_of(6)], emit_joined, s_odd)
    for cp in g_diag[1]:
        cp.wait_recv()
    project_last(0)
    more_chunks([(last, 0)], emit_joined, s_even)
    for cp in g_diag[2]:
        cp.wait_recv()
    project_last(1)
    for cp in last_copies(0):
        cp.wait()
    more_chunks([(last, 1), (UNITS + last, 0)], emit_joined, s_odd)
    k_last, v_last = last_copies(1)
    k_last.wait()
    more_chunks([(UNITS + last, 1)], emit_last, s_even, before_values=v_last.wait)
    add_heads(2)
    for cp in r_first[0]:
        cp.start()
    project_queries(last, 0)

    def join(j):
        for n in quarters:
            span = pl.ds(n * QUARTER, QUARTER)
            r_join[j][n].wait_recv()
            part[4 + j, span, :] += recv[2 + j, span, :]
            r_last[j][n].start()

    def later_unit(i):
        p = (i + 1) // 2
        return 2 * (1 + 2 * ((p + 2) // 3) - p // 2 - 2 * (p // 3)) + lax.rem(i + 1, 2)

    def after_later(i, unit):
        @pl.when((i >= 1) & (i <= 4))
        def _():
            mlp(unit, 0)

        add_heads(unit)

        @pl.when(i == 0)
        def _():
            for cp in r_first[1]:
                cp.start()

        for step in (0, 1):
            @pl.when(i == step + 1)
            def _():
                for n in quarters:
                    r_join[step][n].start()

        @pl.when(i == 4)
        def _():
            join(0)

    attend(7, later_unit, list(range(CHUNKS)), emit_out, after_later)
    join(1)
    for j in (0, 1):
        for half in (0, 1):
            r_first[j][half].wait_recv()
            part[half, parts[j], :] += xg[half, parts[j], :].astype(F32) + recv[j, parts[half], :]
    for j in (0, 1):
        for n in quarters:
            half, start = n // 2, j * HALF + (n % 2) * QUARTER
            r_last[j][n].wait_recv()
            total = part[half, pl.ds(start, QUARTER), :] + recv[4 + j, pl.ds(n * QUARTER, QUARTER), :]
            y_ref[pl.ds(half * ROWS + start, QUARTER), :] = total.astype(BF16)
    for cp in g_copies + w_copies:
        cp.wait_send()
    for group in r_first + r_join + r_last:
        for cp in group:
            cp.wait_send()


def solution(mesh):
    def local_block(x_loc, ln_gamma, w_qkv, w_out, w_up, w_down):
        model_dim = x_loc.shape[1]
        head_dim = w_qkv.shape[2] // 3
        ff = w_up.shape[1]
        head_rows = -(-head_dim // 16) * 16
        hbm = pl.BlockSpec(memory_space=pltpu.HBM)
        vmem = pl.BlockSpec(memory_space=pltpu.VMEM)
        dma = pltpu.SemaphoreType.DMA
        return pl.pallas_call(
            functools.partial(block_kernel, head_dim, head_rows),
            out_shape=pltpu.VMEM(x_loc.shape, BF16),
            in_specs=[hbm, vmem, hbm, hbm, hbm, hbm],
            out_specs=vmem,
            scratch_shapes=[
                pltpu.VMEM((UNITS, ROWS, model_dim), BF16),
                pltpu.VMEM((UNITS, ROWS, model_dim), BF16),
                pltpu.VMEM((2, HEADS, head_rows, model_dim), BF16),
                pltpu.VMEM((HEADS, LANES, model_dim), BF16),
                pltpu.VMEM((HEADS, head_rows, model_dim), BF16),
                pltpu.VMEM((2, ff, model_dim), BF16),
                pltpu.VMEM((2, ff, model_dim), BF16),
                pltpu.VMEM((UNITS, HEADS, LANES, ROWS), BF16),
                pltpu.VMEM((CHUNKS, HEADS, ROWS, LANES), BF16),
                pltpu.VMEM((CHUNKS, HEADS, head_rows, ROWS), BF16),
                pltpu.VMEM((UNITS, ROWS, model_dim), F32),
                pltpu.VMEM((6, ROWS, model_dim), F32),
                pltpu.VMEM((CHUNKS * ROWS, ROWS), F32),
                pltpu.VMEM((CHUNKS * ROWS, ROWS), F32),
                pltpu.VMEM((8, ROWS), F32),
                pltpu.VMEM((8, ROWS), F32),
                pltpu.VMEM((HEADS, head_rows, ROWS), BF16),
                pltpu.VMEM((HEADS, head_rows, ROWS), F32),
                pltpu.VMEM((HEADS, 8, ROWS), F32),
                pltpu.VMEM((HEADS, 8, ROWS), F32),
                pltpu.VMEM((HEADS, 8, ROWS), F32),
                dma((12,)), dma((10,)), dma((10,)), dma((14,)), dma((14,)),
                dma((2, UNITS + 1)), dma((2, UNITS + 1)), dma((20,)), dma((20,)),
            ],
            compiler_params=pltpu.CompilerParams(collective_id=0, has_side_effects=True, vmem_limit_bytes=64000000),
            name="parallel_block",
        )(x_loc, ln_gamma, w_qkv.transpose(1, 2, 0), w_out, w_up.T, w_down)

    row_spec = P(("data", "tp"), None)
    return jax.shard_map(local_block, mesh=mesh, in_specs=(row_spec, P(None), P(None, "tp", None), P("tp", None, None), P(None, "tp"), P("tp", None)), out_specs=row_spec, check_vma=False)
```

```python
import functools
import math
import jax
import jax.numpy as jnp
from jax import lax
from jax.experimental import pallas as pl
from jax.experimental.pallas import tpu as pltpu
from jax.sharding import PartitionSpec as P

LN_EPS = 1e-6
LANES = 128
ROWS = 256
UNITS = 8
CHUNKS = 2 * UNITS
HEADS = 4
HALF = ROWS // 2
QUARTER = ROWS // 4
F32 = jnp.float32
BF16 = jnp.bfloat16
ROW_MAJOR = (((1,), (0,)), ((), ()))
BY_ROWS = (((1,), (1,)), ((), ()))
BY_COLS = (((0,), (0,)), ((), ()))


def dot(a, b, dims=ROW_MAJOR):
    return lax.dot_general(a, b, dims, preferred_element_type=F32)


def gelu_tanh(v):
    return jax.nn.gelu(v, approximate=True)


def block_kernel(head_dim, head_rows, x_hbm, gamma_ref, wqkv_hbm, wout_hbm, w1_hbm, w2_hbm, y_ref,
                 xg, xn, wqv, wk, wout, w1, w2, q_all, k_all, v_all, part, recv, s_even, s_odd, m_even, m_odd, o_t,
                 acc_st, m_st, l_st, m_all,
                 load_sem, wsend, wrecv, gsend, grecv, kvsend, kvrecv, rsend, rrecv):
    me = lax.axis_index("tp")
    core = lax.rem(me, 2)
    chip_x = lax.rem(me // 2, 2)
    chip_y = me // 4
    sib = me + 1 - 2 * core
    x_nbr = me + 2 - 4 * chip_x
    y_nbr = me + 4 - 8 * chip_y
    mesh_id = pl.DeviceIdType.MESH

    def remote(src, dst, send, rcv, dev):
        return pltpu.make_async_remote_copy(src_ref=src, dst_ref=dst, send_sem=send, recv_sem=rcv,
                                            device_id={"tp": dev}, device_id_type=mesh_id)

    loads = [pltpu.make_async_copy(x_hbm.at[pl.ds(half * ROWS, ROWS)], xg.at[half], load_sem.at[half]) for half in (0, 1)]
    for cp in loads:
        cp.start()
    barrier = pltpu.get_barrier_semaphore()

    def greet(dev):
        pl.semaphore_signal(barrier, inc=1, device_id={"tp": dev}, device_id_type=mesh_id)

    greet(x_nbr)
    greet(y_nbr)
    wqv[:, :, head_rows - 16:, :] = jnp.zeros((2, HEADS, 16, wqv.shape[3]), BF16)
    wk[:, LANES - 64:, :] = jnp.zeros((HEADS, 64, wk.shape[2]), BF16)
    wout[:, head_rows - 16:, :] = jnp.zeros((HEADS, 16, wout.shape[2]), BF16)
    greet(sib)

    pairs = []
    for hh in (0, 1):
        h = 2 * core + hh
        real = pl.ds(0, head_dim)
        pairs += [
            (wqkv_hbm.at[hh, pl.ds(0, head_dim)], wqv.at[0, h, real]),
            (wqkv_hbm.at[hh, pl.ds(head_dim, head_dim)], wk.at[h, real]),
            (wqkv_hbm.at[hh, pl.ds(2 * head_dim, head_dim)], wqv.at[1, h, real]),
            (wout_hbm.at[hh], wout.at[h, real]),
        ]
    pairs += [(w1_hbm, w1.at[core]), (w2_hbm, w2.at[core])]

    pl.semaphore_wait(barrier, 3)

    top, low = pl.ds(0, HALF), pl.ds(HALF, HALF)
    parts = (top, low)

    def diag_copy(src, dst, span, idx, dev):
        return remote(xn.at[src, span], xn.at[dst, span], gsend.at[idx], grecv.at[idx], dev)

    def own(half, j):
        return x_hbm.at[pl.ds(half * ROWS + j * HALF, HALF)]

    g_first = [(remote(own(0, j), xg.at[2 + j, top], gsend.at[j], grecv.at[j], y_nbr), remote(own(1, j), xg.at[2 + j, low], gsend.at[2 + j], grecv.at[2 + j], x_nbr)) for j in (0, 1)]
    g_second = [(remote(own(0, j), xg.at[4 + j, top], gsend.at[4 + j], grecv.at[4 + j], x_nbr), remote(own(1, j), xg.at[4 + j, low], gsend.at[6 + j], grecv.at[6 + j], y_nbr)) for j in (0, 1)]
    g_diag = [(diag_copy(2, 6, top, 8, x_nbr), diag_copy(2, 6, low, 9, y_nbr))]
    for q in (0, 1):
        q_top, q_low = pl.ds(q * QUARTER, QUARTER), pl.ds(HALF + q * QUARTER, QUARTER)
        g_diag.append((diag_copy(3, 7, q_top, 10 + q, x_nbr), diag_copy(3, 7, q_low, 12 + q, y_nbr)))
    g_copies = [cp for group in (g_first, g_second, g_diag) for two in group for cp in two]
    for cp in g_copies[:8]:
        cp.start()
    w_copies = [remote(src, dst, wsend.at[n], wrecv.at[n], sib) for n, (src, dst) in enumerate(pairs)]
    w_loads = [pltpu.make_async_copy(src, dst, load_sem.at[2 + n]) for n, (src, dst) in enumerate(pairs)]
    for cp in w_copies + w_loads:
        cp.start()

    zero_rows = LANES - head_rows

    def clear(unit, _):
        q_all[unit, :, head_rows:, :] = jnp.zeros((HEADS, zero_rows, ROWS), BF16)
        return 0

    lax.fori_loop(0, UNITS, clear, 0)

    def kv_copies(unit):
        return (
            remote(k_all.at[unit], k_all.at[UNITS + unit], kvsend.at[0, unit], kvrecv.at[0, unit], sib),
            remote(v_all.at[unit], v_all.at[UNITS + unit], kvsend.at[1, unit], kvrecv.at[1, unit], sib),
        )

    def normalize(rows):
        rows = rows.astype(F32)
        mean = jnp.mean(rows, axis=-1, keepdims=True)
        cent = rows - mean
        var = jnp.mean(cent * cent, axis=-1, keepdims=True)
        return (cent * lax.rsqrt(var + LN_EPS) * gamma_ref[...][None, :]).astype(BF16)

    last = UNITS - 1

    def last_copies(q):
        span = parts[q]
        return (
            remote(k_all.at[last, :, span], k_all.at[UNITS + last, :, span], kvsend.at[q, last], kvrecv.at[q, last], sib),
            remote(v_all.at[last, :, :, span], v_all.at[UNITS + last, :, :, span], kvsend.at[q, UNITS], kvrecv.at[q, UNITS], sib),
        )

    def project_last(q):
        spans = (pl.ds(q * QUARTER, QUARTER), pl.ds(HALF + q * QUARTER, QUARTER))
        normed = jnp.concatenate([xn[last, span] for span in spans], axis=0)
        keys = dot(normed, wk[...].reshape(HEADS * LANES, -1), BY_ROWS)
        for h in range(HEADS):
            k_all[last, h, parts[q]] = keys[:, h * LANES:(h + 1) * LANES].astype(BF16)
        k_copy, v_copy = last_copies(q)
        k_copy.start()
        values = dot(wqv[1].reshape(HEADS * head_rows, -1), normed, BY_ROWS).astype(BF16)
        for h in range(HEADS):
            v_all[last, h, :, parts[q]] = values[h * head_rows:(h + 1) * head_rows]
        v_copy.start()

    def project(unit, _):
        normed = normalize(xg[unit])
        xn[unit] = normed
        return keys_values(unit, normed)

    def keys_values(unit, normed):
        keys = dot(normed, wk[...].reshape(HEADS * LANES, -1), BY_ROWS)
        for h in range(HEADS):
            k_all[unit, h] = keys[:, h * LANES:(h + 1) * LANES].astype(BF16)
        k_copy, v_copy = kv_copies(unit)
        k_copy.start()
        values = dot(wqv[1].reshape(HEADS * head_rows, -1), normed, BY_ROWS).astype(BF16)
        for h in range(HEADS):
            v_all[unit, h] = values[h * head_rows:(h + 1) * head_rows]
        v_copy.start()
        return 0

    def project_queries(unit, _):
        queries = dot(wqv[0].reshape(HEADS * head_rows, -1), xn[unit], BY_ROWS).astype(BF16)
        for h in range(HEADS):
            q_all[unit, h, :head_rows] = queries[h * head_rows:(h + 1) * head_rows]
        return 0

    def project_both(unit, _):
        project(unit, 0)
        return project_queries(unit, 0)

    def mlp(unit, _):
        rows = xn[unit]
        total = None
        for s in (0, 1):
            hidden = gelu_tanh(dot(rows, w1[s], BY_ROWS)).astype(BF16)
            term = dot(hidden, w2[s])
            total = term if total is None else total + term
        part[unit] = total
        return 0

    def kv_wait(unit, _):
        for cp in kv_copies(unit):
            cp.wait()
        return 0

    exp_scale = (head_dim ** -0.5) * math.log2(math.e)
    groups = ROWS // 8

    def chunks_of(*units):
        return list(units) + [UNITS + u for u in units]


    def score_chunk(n, c, h, q, s_ref):
        s = dot(k_all[c, h], q)
        s_ref[pl.ds(n * ROWS, ROWS), :] = s
        return jnp.max(s.reshape(groups, 8, ROWS), axis=0)

    def finish(chunks, h, s_ref, m_ref, unit_n, h_n, s_next, m_next):
        q_n = q_all[unit_n, h_n]
        m = jnp.max(m_ref[...], axis=0, keepdims=True)
        acc = None
        total = None
        m_n = None
        for n, c in enumerate(chunks):
            mc = score_chunk(n, c, h_n, q_n, s_next)
            m_n = mc if m_n is None else jnp.maximum(m_n, mc)
            e = jnp.exp2((s_ref[pl.ds(n * ROWS, ROWS), :] - m) * exp_scale)
            tc = jnp.sum(e.reshape(groups, 8, ROWS), axis=0)
            total = tc if total is None else total + tc
            pv = dot(v_all[c, h], e.astype(BF16))
            acc = pv if acc is None else acc + pv
        m_next[...] = m_n
        return m, jnp.sum(total, axis=0, keepdims=True), acc

    def attend(count, unit_of, chunks, emit, after):
        q = q_all[unit_of(0), 0]
        m = None
        for n, c in enumerate(chunks):
            mc = score_chunk(n, c, 0, q, s_even)
            m = mc if m is None else jnp.maximum(m, mc)
        m_even[...] = m

        def one(i, _):
            unit = unit_of(i)
            unit_next = unit_of(lax.rem(i + 1, count))

            def pair(p, _):
                emit(i, 2 * p, *finish(chunks, 2 * p, s_even, m_even, unit, 2 * p + 1, s_odd, m_odd))
                follow = unit + p * (unit_next - unit)
                emit(i, 2 * p + 1, *finish(chunks, 2 * p + 1, s_odd, m_odd, follow, 2 - 2 * p, s_even, m_even))
                return 0

            lax.fori_loop(0, 2, pair, 0)
            after(i, unit)
            return 0

        lax.fori_loop(0, count, one, 0)

    def emit_state(i, h, m, total, acc):
        m_st[h] = jnp.broadcast_to(m, m_st.shape[1:])
        l_st[h] = jnp.broadcast_to(total, l_st.shape[1:])
        acc_st[h] = acc

    def more_chunks(pieces, emit, s_ref, before_values=None):
        size = ROWS if pieces[0][1] is None else HALF

        def rows_of(h, n):
            return pl.ds((h * len(pieces) + n) * size, size)

        for h in range(HEADS):
            q = q_all[2, h]
            m = None
            for n, (c, part_no) in enumerate(pieces):
                s = dot(k_all[c, h] if part_no is None else k_all[c, h, parts[part_no]], q)
                s_ref[rows_of(h, n), :] = s
                mc = jnp.max(s.reshape(size // 8, 8, ROWS), axis=0)
                m = mc if m is None else jnp.maximum(m, mc)
            m_all[h] = m
        if before_values is not None:
            before_values()
        for h in range(HEADS):
            m = jnp.max(m_all[h], axis=0, keepdims=True)
            total = None
            acc = None
            for n, (c, part_no) in enumerate(pieces):
                e = jnp.exp2((s_ref[rows_of(h, n), :] - m) * exp_scale)
                tc = jnp.sum(e.reshape(size // 8, 8, ROWS), axis=0)
                total = tc if total is None else total + tc
                v = v_all[c, h] if part_no is None else v_all[c, h, :, parts[part_no]]
                pv = dot(v, e.astype(BF16))
                acc = pv if acc is None else acc + pv
            emit(0, h, m, jnp.sum(total, axis=0, keepdims=True), acc)

    def joined(h, m, total, acc):
        m_old = m_st[h][:1]
        high = jnp.maximum(m, m_old)
        a_new = jnp.exp2((m - high) * exp_scale)
        a_old = jnp.exp2((m_old - high) * exp_scale)
        return high, total * a_new + l_st[h][:1] * a_old, acc * a_new + acc_st[h] * a_old

    def emit_joined(i, h, m, total, acc):
        emit_state(i, h, *joined(h, m, total, acc))

    def emit_last(i, h, m, total, acc):
        emit_out(i, h, *joined(h, m, total, acc))

    def emit_out(i, h, m, total, acc):
        o_t[h] = (acc / total).astype(BF16)

    def add_heads(unit):
        part[unit] += dot(o_t[...].reshape(HEADS * head_rows, ROWS), wout[...].reshape(HEADS * head_rows, -1), BY_COLS)

    def reduce_copy(src, dst, start, size, sem, dev):
        span = pl.ds(start, size)
        return remote(part.at[src, span], recv.at[dst, span], rsend.at[sem], rrecv.at[sem], dev)

    r_first = [(reduce_copy(2 + j, j, 0, HALF, 2 * j, y_nbr), reduce_copy(2 + j, j, HALF, HALF, 2 * j + 1, x_nbr)) for j in (0, 1)]
    quarters = (0, 2, 1, 3)

    def quarter_copies(src, dst, sem, first, second):
        return [reduce_copy(src, dst, n * QUARTER, QUARTER, sem + n, first if n < 2 else second) for n in range(4)]

    r_join = [quarter_copies(6 + j, 2 + j, 4 + 4 * j, y_nbr, x_nbr) for j in (0, 1)]
    r_last = [quarter_copies(4 + j, 4 + j, 12 + 4 * j, x_nbr, y_nbr) for j in (0, 1)]

    for cp in loads + w_loads:
        cp.wait()
    for cp in w_copies:
        cp.wait_recv()
    lax.fori_loop(0, 2, project_both, 0)
    lax.fori_loop(0, 2, mlp, 0)
    for j in (0, 1):
        for cp in g_first[j]:
            cp.wait_recv()
        project_both(2 + j, 0)
        for two in g_diag[:1] if j == 0 else g_diag[1:]:
            for cp in two:
                cp.start()
    lax.fori_loop(0, 4, kv_wait, 0)
    attend(1, lambda i: 2, chunks_of(0, 1, 2, 3), emit_state, lambda i, unit: None)
    lax.fori_loop(2, 4, mlp, 0)
    for j in (0, 1):
        for cp in g_second[j]:
            cp.wait_recv()
    lax.fori_loop(4, 6, project_both, 0)
    lax.fori_loop(4, 6, kv_wait, 0)
    more_chunks([(c, None) for c in chunks_of(4, 5)], emit_joined, s_even)
    for cp in g_diag[0]:
        cp.wait_recv()
    keys_values(6, xn[6])
    project_queries(6, 0)
    kv_wait(6, 0)
    more_chunks([(c, None) for c in chunks_of(6)], emit_joined, s_odd)
    for cp in g_diag[1]:
        cp.wait_recv()
    project_last(0)
    more_chunks([(last, 0)], emit_joined, s_even)
    for cp in g_diag[2]:
        cp.wait_recv()
    project_last(1)
    for cp in last_copies(0):
        cp.wait()
    more_chunks([(last, 1), (UNITS + last, 0)], emit_joined, s_odd)
    k_last, v_last = last_copies(1)
    k_last.wait()
    more_chunks([(UNITS + last, 1)], emit_last, s_even, before_values=v_last.wait)
    add_heads(2)
    for cp in r_first[0]:
        cp.start()
    project_queries(last, 0)

    def join(j):
        for n in quarters:
            span = pl.ds(n * QUARTER, QUARTER)
            r_join[j][n].wait_recv()
            part[4 + j, span, :] += recv[2 + j, span, :]
            r_last[j][n].start()

    def later_unit(i):
        p = (i + 1) // 2
        return 2 * (1 + 2 * ((p + 2) // 3) - p // 2 - 2 * (p // 3)) + lax.rem(i + 1, 2)

    def after_later(i, unit):
        @pl.when((i >= 1) & (i <= 4))
        def _():
            mlp(unit, 0)

        add_heads(unit)

        @pl.when(i == 0)
        def _():
            for cp in r_first[1]:
                cp.start()

        for step in (0, 1):
            @pl.when(i == step + 1)
            def _():
                for n in quarters:
                    r_join[step][n].start()

        @pl.when(i == 4)
        def _():
            join(0)

    attend(7, later_unit, list(range(CHUNKS)), emit_out, after_later)
    join(1)
    for j in (0, 1):
        for half in (0, 1):
            r_first[j][half].wait_recv()
            part[half, parts[j], :] += xg[half, parts[j], :].astype(F32) + recv[j, parts[half], :]
    for j in (0, 1):
        for n in quarters:
            half, start = n // 2, j * HALF + (n % 2) * QUARTER
            r_last[j][n].wait_recv()
            total = part[half, pl.ds(start, QUARTER), :] + recv[4 + j, pl.ds(n * QUARTER, QUARTER), :]
            y_ref[pl.ds(half * ROWS + start, QUARTER), :] = total.astype(BF16)
    for cp in g_copies + w_copies:
        cp.wait_send()
    for group in r_first + r_join + r_last:
        for cp in group:
            cp.wait_send()


def solution(mesh):
    def local_block(x_loc, ln_gamma, w_qkv, w_out, w_up, w_down):
        model_dim = x_loc.shape[1]
        head_dim = w_qkv.shape[2] // 3
        ff = w_up.shape[1]
        head_rows = -(-head_dim // 16) * 16
        hbm = pl.BlockSpec(memory_space=pltpu.HBM)
        vmem = pl.BlockSpec(memory_space=pltpu.VMEM)
        dma = pltpu.SemaphoreType.DMA
        return pl.pallas_call(
            functools.partial(block_kernel, head_dim, head_rows),
            out_shape=pltpu.VMEM(x_loc.shape, BF16),
            in_specs=[hbm, vmem, hbm, hbm, hbm, hbm],
            out_specs=vmem,
            scratch_shapes=[
                pltpu.VMEM((UNITS - 2, ROWS, model_dim), BF16),
                pltpu.VMEM((UNITS, ROWS, model_dim), BF16),
                pltpu.VMEM((2, HEADS, head_rows, model_dim), BF16),
                pltpu.VMEM((HEADS, LANES, model_dim), BF16),
                pltpu.VMEM((HEADS, head_rows, model_dim), BF16),
                pltpu.VMEM((2, ff, model_dim), BF16),
                pltpu.VMEM((2, ff, model_dim), BF16),
                pltpu.VMEM((UNITS, HEADS, LANES, ROWS), BF16),
                pltpu.VMEM((CHUNKS, HEADS, ROWS, LANES), BF16),
                pltpu.VMEM((CHUNKS, HEADS, head_rows, ROWS), BF16),
                pltpu.VMEM((UNITS, ROWS, model_dim), F32),
                pltpu.VMEM((6, ROWS, model_dim), F32),
                pltpu.VMEM((CHUNKS * ROWS, ROWS), F32),
                pltpu.VMEM((CHUNKS * ROWS, ROWS), F32),
                pltpu.VMEM((8, ROWS), F32),
                pltpu.VMEM((8, ROWS), F32),
                pltpu.VMEM((HEADS, head_rows, ROWS), BF16),
                pltpu.VMEM((HEADS, head_rows, ROWS), F32),
                pltpu.VMEM((HEADS, 8, ROWS), F32),
                pltpu.VMEM((HEADS, 8, ROWS), F32),
                pltpu.VMEM((HEADS, 8, ROWS), F32),
                dma((12,)), dma((10,)), dma((10,)), dma((14,)), dma((14,)),
                dma((2, UNITS + 1)), dma((2, UNITS + 1)), dma((20,)), dma((20,)),
            ],
            compiler_params=pltpu.CompilerParams(collective_id=0, has_side_effects=True, vmem_limit_bytes=64000000),
            name="parallel_block",
        )(x_loc, ln_gamma, w_qkv.transpose(1, 2, 0), w_out, w_up.T, w_down)

    row_spec = P(("data", "tp"), None)
    return jax.shard_map(local_block, mesh=mesh, in_specs=(row_spec, P(None), P(None, "tp", None), P("tp", None, None), P(None, "tp"), P("tp", None)), out_specs=row_spec, check_vma=False)
```

```python
import functools
import math
import jax
import jax.numpy as jnp
from jax import lax
from jax.experimental import pallas as pl
from jax.experimental.pallas import tpu as pltpu
from jax.sharding import PartitionSpec as P

LN_EPS = 1e-6
LANES = 128
ROWS = 256
UNITS = 8
CHUNKS = 2 * UNITS
HEADS = 4
HALF = ROWS // 2
QUARTER = ROWS // 4
F32 = jnp.float32
BF16 = jnp.bfloat16
ROW_MAJOR = (((1,), (0,)), ((), ()))
BY_ROWS = (((1,), (1,)), ((), ()))
BY_COLS = (((0,), (0,)), ((), ()))


def dot(a, b, dims=ROW_MAJOR):
    return lax.dot_general(a, b, dims, preferred_element_type=F32)


def gelu_tanh(v):
    return jax.nn.gelu(v, approximate=True)


def block_kernel(head_dim, head_rows, x_hbm, gamma_ref, wqkv_hbm, wout_hbm, w1_hbm, w2_hbm, y_ref,
                 xg, xn, wqv, wk, wk_t, wout, w1, w2, q_all, k_all, v_all, part, recv, s_even, s_odd, m_even, m_odd, o_t,
                 acc_st, m_st, l_st, m_all,
                 load_sem, pad_sem, wsend, wrecv, gsend, grecv, kvsend, kvrecv, rsend, rrecv):
    me = lax.axis_index("tp")
    core = lax.rem(me, 2)
    chip_x = lax.rem(me // 2, 2)
    chip_y = me // 4
    sib = me + 1 - 2 * core
    x_nbr = me + 2 - 4 * chip_x
    y_nbr = me + 4 - 8 * chip_y
    mesh_id = pl.DeviceIdType.MESH

    def remote(src, dst, send, rcv, dev):
        return pltpu.make_async_remote_copy(src_ref=src, dst_ref=dst, send_sem=send, recv_sem=rcv,
                                            device_id={"tp": dev}, device_id_type=mesh_id)

    barrier = pltpu.get_barrier_semaphore()
    for dev in (x_nbr, y_nbr, sib):
        pl.semaphore_signal(barrier, inc=1, device_id={"tp": dev}, device_id_type=mesh_id)
    loads = [pltpu.make_async_copy(x_hbm.at[pl.ds(half * ROWS, ROWS)], xg.at[half], load_sem.at[half]) for half in (0, 1)]

    pairs = []
    for hh in (0, 1):
        h = 2 * core + hh
        real = pl.ds(0, head_dim)
        pairs += [
            (wqkv_hbm.at[hh, pl.ds(0, head_dim)], wqv.at[0, h, real]),
            (wqkv_hbm.at[hh, pl.ds(head_dim, head_dim)], wk.at[h, real]),
            (wqkv_hbm.at[hh, pl.ds(2 * head_dim, head_dim)], wqv.at[1, h, real]),
            (wout_hbm.at[hh], wout.at[h, real]),
        ]
    pairs += [(w1_hbm, w1.at[core]), (w2_hbm, w2.at[core])]

    pl.semaphore_wait(barrier, 3)

    top, low = pl.ds(0, HALF), pl.ds(HALF, HALF)
    parts = (top, low)

    def diag_copy(src, dst, span, idx, dev):
        return remote(xn.at[src, span], xn.at[dst, span], gsend.at[idx], grecv.at[idx], dev)

    def own(half, j):
        return x_hbm.at[pl.ds(half * ROWS + j * HALF, HALF)]

    g_first = [(remote(own(0, j), xg.at[2 + j, top], gsend.at[j], grecv.at[j], y_nbr), remote(own(1, j), xg.at[2 + j, low], gsend.at[2 + j], grecv.at[2 + j], x_nbr)) for j in (0, 1)]
    g_second = [(remote(own(0, j), xg.at[4 + j, top], gsend.at[4 + j], grecv.at[4 + j], x_nbr), remote(own(1, j), xg.at[4 + j, low], gsend.at[6 + j], grecv.at[6 + j], y_nbr)) for j in (0, 1)]
    g_diag = [(diag_copy(2, 6, top, 8, x_nbr), diag_copy(2, 6, low, 9, y_nbr))]
    for q in (0, 1):
        q_top, q_low = pl.ds(q * QUARTER, QUARTER), pl.ds(HALF + q * QUARTER, QUARTER)
        g_diag.append((diag_copy(3, 7, q_top, 10 + q, x_nbr), diag_copy(3, 7, q_low, 12 + q, y_nbr)))
    g_copies = [cp for group in (g_first, g_second, g_diag) for two in group for cp in two]
    for cp in g_copies[:8] + loads:
        cp.start()
    wqv[:, :, head_rows - 16:, :] = jnp.zeros((2, HEADS, 16, wqv.shape[3]), BF16)
    wk[:, LANES - 64:, :] = jnp.zeros((HEADS, 64, wk.shape[2]), BF16)
    wout[:, head_rows - 16:, :] = jnp.zeros((HEADS, 16, wout.shape[2]), BF16)
    pl.semaphore_signal(pad_sem, inc=1, device_id={"tp": sib}, device_id_type=mesh_id)
    pl.semaphore_wait(pad_sem, 1)
    w_copies = [remote(src, dst, wsend.at[n], wrecv.at[n], sib) for n, (src, dst) in enumerate(pairs)]
    w_loads = [pltpu.make_async_copy(src, dst, load_sem.at[2 + n]) for n, (src, dst) in enumerate(pairs)]
    for cp in w_copies + w_loads:
        cp.start()

    zero_rows = LANES - head_rows

    def clear(unit, _):
        q_all[unit, :, head_rows:, :] = jnp.zeros((HEADS, zero_rows, ROWS), BF16)
        return 0

    lax.fori_loop(0, UNITS, clear, 0)

    def kv_copies(unit):
        return (
            remote(k_all.at[unit], k_all.at[UNITS + unit], kvsend.at[0, unit], kvrecv.at[0, unit], sib),
            remote(v_all.at[unit], v_all.at[UNITS + unit], kvsend.at[1, unit], kvrecv.at[1, unit], sib),
        )

    def normalize(rows):
        rows = rows.astype(F32)
        mean = jnp.mean(rows, axis=-1, keepdims=True)
        cent = rows - mean
        var = jnp.mean(cent * cent, axis=-1, keepdims=True)
        return (cent * lax.rsqrt(var + LN_EPS) * gamma_ref[...][None, :]).astype(BF16)

    last = UNITS - 1

    def last_copies(q):
        span = parts[q]
        return (
            remote(k_all.at[last, :, span], k_all.at[UNITS + last, :, span], kvsend.at[q, last], kvrecv.at[q, last], sib),
            remote(v_all.at[last, :, :, span], v_all.at[UNITS + last, :, :, span], kvsend.at[q, UNITS], kvrecv.at[q, UNITS], sib),
        )

    def project_last(q):
        spans = (pl.ds(q * QUARTER, QUARTER), pl.ds(HALF + q * QUARTER, QUARTER))
        normed = jnp.concatenate([xn[last, span] for span in spans], axis=0)
        keys = dot(normed, wk_t[...])
        for h in range(HEADS):
            k_all[last, h, parts[q]] = keys[:, h * LANES:(h + 1) * LANES].astype(BF16)
        k_copy, v_copy = last_copies(q)
        k_copy.start()
        values = dot(wqv[1].reshape(HEADS * head_rows, -1), normed, BY_ROWS).astype(BF16)
        for h in range(HEADS):
            v_all[last, h, :, parts[q]] = values[h * head_rows:(h + 1) * head_rows]
        v_copy.start()

    def project(unit, _):
        normed = normalize(xg[unit])
        xn[unit] = normed
        return keys_values(unit, normed)

    def keys_values(unit, normed):
        keys = dot(normed, wk_t[...])
        for h in range(HEADS):
            k_all[unit, h] = keys[:, h * LANES:(h + 1) * LANES].astype(BF16)
        k_copy, v_copy = kv_copies(unit)
        k_copy.start()
        values = dot(wqv[1].reshape(HEADS * head_rows, -1), normed, BY_ROWS).astype(BF16)
        for h in range(HEADS):
            v_all[unit, h] = values[h * head_rows:(h + 1) * head_rows]
        v_copy.start()
        return 0

    def project_queries(unit, _):
        queries = dot(wqv[0].reshape(HEADS * head_rows, -1), xn[unit], BY_ROWS).astype(BF16)
        for h in range(HEADS):
            q_all[unit, h, :head_rows] = queries[h * head_rows:(h + 1) * head_rows]
        return 0

    def project_both(unit, _):
        project(unit, 0)
        return project_queries(unit, 0)

    def mlp(unit, _):
        rows = xn[unit]
        total = None
        for s in (0, 1):
            hidden = gelu_tanh(dot(rows, w1[s], BY_ROWS)).astype(BF16)
            term = dot(hidden, w2[s])
            total = term if total is None else total + term
        part[unit] = total
        return 0

    def kv_wait(unit, _):
        for cp in kv_copies(unit):
            cp.wait()
        return 0

    exp_scale = (head_dim ** -0.5) * math.log2(math.e)
    groups = ROWS // 8

    def chunks_of(*units):
        return list(units) + [UNITS + u for u in units]


    def score_chunk(n, c, h, q, s_ref):
        s = dot(k_all[c, h], q)
        s_ref[pl.ds(n * ROWS, ROWS), :] = s
        return jnp.max(s.reshape(groups, 8, ROWS), axis=0)

    def finish(chunks, h, s_ref, m_ref, unit_n, h_n, s_next, m_next):
        q_n = q_all[unit_n, h_n]
        m = jnp.max(m_ref[...], axis=0, keepdims=True)
        acc = None
        total = None
        m_n = None
        for n, c in enumerate(chunks):
            mc = score_chunk(n, c, h_n, q_n, s_next)
            m_n = mc if m_n is None else jnp.maximum(m_n, mc)
            e = jnp.exp2((s_ref[pl.ds(n * ROWS, ROWS), :] - m) * exp_scale)
            tc = jnp.sum(e.reshape(groups, 8, ROWS), axis=0)
            total = tc if total is None else total + tc
            pv = dot(v_all[c, h], e.astype(BF16))
            acc = pv if acc is None else acc + pv
        m_next[...] = m_n
        return m, jnp.sum(total, axis=0, keepdims=True), acc

    def attend(count, unit_of, chunks, emit, after):
        q = q_all[unit_of(0), 0]
        m = None
        for n, c in enumerate(chunks):
            mc = score_chunk(n, c, 0, q, s_even)
            m = mc if m is None else jnp.maximum(m, mc)
        m_even[...] = m

        def one(i, _):
            unit = unit_of(i)
            unit_next = unit_of(lax.rem(i + 1, count))

            def pair(p, _):
                emit(i, 2 * p, *finish(chunks, 2 * p, s_even, m_even, unit, 2 * p + 1, s_odd, m_odd))
                follow = unit + p * (unit_next - unit)
                emit(i, 2 * p + 1, *finish(chunks, 2 * p + 1, s_odd, m_odd, follow, 2 - 2 * p, s_even, m_even))
                return 0

            lax.fori_loop(0, 2, pair, 0)
            after(i, unit)
            return 0

        lax.fori_loop(0, count, one, 0)

    def emit_state(i, h, m, total, acc):
        m_st[h] = jnp.broadcast_to(m, m_st.shape[1:])
        l_st[h] = jnp.broadcast_to(total, l_st.shape[1:])
        acc_st[h] = acc

    def more_chunks(pieces, emit, s_ref, before_values=None):
        size = ROWS if pieces[0][1] is None else HALF

        def rows_of(h, n):
            return pl.ds((h * len(pieces) + n) * size, size)

        for h in range(HEADS):
            q = q_all[2, h]
            m = None
            for n, (c, part_no) in enumerate(pieces):
                s = dot(k_all[c, h] if part_no is None else k_all[c, h, parts[part_no]], q)
                s_ref[rows_of(h, n), :] = s
                mc = jnp.max(s.reshape(size // 8, 8, ROWS), axis=0)
                m = mc if m is None else jnp.maximum(m, mc)
            m_all[h] = m
        if before_values is not None:
            before_values()
        for h in range(HEADS):
            m = jnp.max(m_all[h], axis=0, keepdims=True)
            total = None
            acc = None
            for n, (c, part_no) in enumerate(pieces):
                e = jnp.exp2((s_ref[rows_of(h, n), :] - m) * exp_scale)
                tc = jnp.sum(e.reshape(size // 8, 8, ROWS), axis=0)
                total = tc if total is None else total + tc
                v = v_all[c, h] if part_no is None else v_all[c, h, :, parts[part_no]]
                pv = dot(v, e.astype(BF16))
                acc = pv if acc is None else acc + pv
            emit(0, h, m, jnp.sum(total, axis=0, keepdims=True), acc)

    def joined(h, m, total, acc):
        m_old = m_st[h][:1]
        high = jnp.maximum(m, m_old)
        a_new = jnp.exp2((m - high) * exp_scale)
        a_old = jnp.exp2((m_old - high) * exp_scale)
        return high, total * a_new + l_st[h][:1] * a_old, acc * a_new + acc_st[h] * a_old

    def emit_joined(i, h, m, total, acc):
        emit_state(i, h, *joined(h, m, total, acc))

    def emit_last(i, h, m, total, acc):
        emit_out(i, h, *joined(h, m, total, acc))

    def emit_out(i, h, m, total, acc):
        o_t[h] = (acc / total).astype(BF16)

    def add_heads(unit):
        part[unit] += dot(o_t[...].reshape(HEADS * head_rows, ROWS), wout[...].reshape(HEADS * head_rows, -1), BY_COLS)

    def reduce_copy(src, dst, start, size, sem, dev):
        span = pl.ds(start, size)
        return remote(part.at[src, span], recv.at[dst, span], rsend.at[sem], rrecv.at[sem], dev)

    r_first = [(reduce_copy(2 + j, j, 0, HALF, 2 * j, y_nbr), reduce_copy(2 + j, j, HALF, HALF, 2 * j + 1, x_nbr)) for j in (0, 1)]
    quarters = (0, 2, 1, 3)

    def quarter_copies(src, dst, sem, first, second):
        return [reduce_copy(src, dst, n * QUARTER, QUARTER, sem + n, first if n < 2 else second) for n in range(4)]

    r_join = [quarter_copies(6 + j, 2 + j, 4 + 4 * j, y_nbr, x_nbr) for j in (0, 1)]
    r_last = [quarter_copies(4 + j, 4 + j, 12 + 4 * j, x_nbr, y_nbr) for j in (0, 1)]

    for cp in loads + w_loads:
        cp.wait()
    for cp in w_copies:
        cp.wait_recv()
    for h in range(HEADS):
        wk_t[:, h * LANES:(h + 1) * LANES] = jnp.transpose(wk[h])
    lax.fori_loop(0, 2, project_both, 0)
    lax.fori_loop(0, 2, mlp, 0)
    for j in (0, 1):
        for cp in g_first[j]:
            cp.wait_recv()
        project_both(2 + j, 0)
        for two in g_diag[:1] if j == 0 else g_diag[1:]:
            for cp in two:
                cp.start()
    lax.fori_loop(0, 4, kv_wait, 0)
    attend(1, lambda i: 2, chunks_of(0, 1, 2, 3), emit_state, lambda i, unit: None)
    lax.fori_loop(2, 4, mlp, 0)
    for j in (0, 1):
        for cp in g_second[j]:
            cp.wait_recv()
    lax.fori_loop(4, 6, project_both, 0)
    lax.fori_loop(4, 6, kv_wait, 0)
    more_chunks([(c, None) for c in chunks_of(4, 5)], emit_joined, s_even)
    for cp in g_diag[0]:
        cp.wait_recv()
    keys_values(6, xn[6])
    project_queries(6, 0)
    kv_wait(6, 0)
    more_chunks([(c, None) for c in chunks_of(6)], emit_joined, s_odd)
    for cp in g_diag[1]:
        cp.wait_recv()
    project_last(0)
    more_chunks([(last, 0)], emit_joined, s_even)
    for cp in g_diag[2]:
        cp.wait_recv()
    project_last(1)
    for cp in last_copies(0):
        cp.wait()
    more_chunks([(last, 1), (UNITS + last, 0)], emit_joined, s_odd)
    k_last, v_last = last_copies(1)
    k_last.wait()
    more_chunks([(UNITS + last, 1)], emit_last, s_even, before_values=v_last.wait)
    add_heads(2)
    for cp in r_first[0]:
        cp.start()
    project_queries(last, 0)

    def join(j):
        for n in quarters:
            span = pl.ds(n * QUARTER, QUARTER)
            r_join[j][n].wait_recv()
            part[4 + j, span, :] += recv[2 + j, span, :]
            r_last[j][n].start()

    def later_unit(i):
        p = (i + 1) // 2
        return 2 * (1 + 2 * ((p + 2) // 3) - p // 2 - 2 * (p // 3)) + lax.rem(i + 1, 2)

    def after_later(i, unit):
        @pl.when((i >= 1) & (i <= 4))
        def _():
            mlp(unit, 0)

        add_heads(unit)

        @pl.when(i == 0)
        def _():
            for cp in r_first[1]:
                cp.start()

        for step in (0, 1):
            @pl.when(i == step + 1)
            def _():
                for n in quarters:
                    r_join[step][n].start()

        @pl.when(i == 4)
        def _():
            join(0)

    attend(7, later_unit, list(range(CHUNKS)), emit_out, after_later)
    join(1)
    for j in (0, 1):
        for half in (0, 1):
            r_first[j][half].wait_recv()
            part[half, parts[j], :] += xg[half, parts[j], :].astype(F32) + recv[j, parts[half], :]
    for j in (0, 1):
        for n in quarters:
            half, start = n // 2, j * HALF + (n % 2) * QUARTER
            r_last[j][n].wait_recv()
            total = part[half, pl.ds(start, QUARTER), :] + recv[4 + j, pl.ds(n * QUARTER, QUARTER), :]
            y_ref[pl.ds(half * ROWS + start, QUARTER), :] = total.astype(BF16)
    for cp in g_copies + w_copies:
        cp.wait_send()
    for group in r_first + r_join + r_last:
        for cp in group:
            cp.wait_send()


def solution(mesh):
    def local_block(x_loc, ln_gamma, w_qkv, w_out, w_up, w_down):
        model_dim = x_loc.shape[1]
        head_dim = w_qkv.shape[2] // 3
        ff = w_up.shape[1]
        head_rows = -(-head_dim // 16) * 16
        hbm = pl.BlockSpec(memory_space=pltpu.HBM)
        vmem = pl.BlockSpec(memory_space=pltpu.VMEM)
        dma = pltpu.SemaphoreType.DMA
        return pl.pallas_call(
            functools.partial(block_kernel, head_dim, head_rows),
            out_shape=pltpu.VMEM(x_loc.shape, BF16),
            in_specs=[hbm, vmem, hbm, hbm, hbm, hbm],
            out_specs=vmem,
            scratch_shapes=[
                pltpu.VMEM((UNITS - 2, ROWS, model_dim), BF16),
                pltpu.VMEM((UNITS, ROWS, model_dim), BF16),
                pltpu.VMEM((2, HEADS, head_rows, model_dim), BF16),
                pltpu.VMEM((HEADS, LANES, model_dim), BF16),
                pltpu.VMEM((model_dim, HEADS * LANES), BF16),
                pltpu.VMEM((HEADS, head_rows, model_dim), BF16),
                pltpu.VMEM((2, ff, model_dim), BF16),
                pltpu.VMEM((2, ff, model_dim), BF16),
                pltpu.VMEM((UNITS, HEADS, LANES, ROWS), BF16),
                pltpu.VMEM((CHUNKS, HEADS, ROWS, LANES), BF16),
                pltpu.VMEM((CHUNKS, HEADS, head_rows, ROWS), BF16),
                pltpu.VMEM((UNITS, ROWS, model_dim), F32),
                pltpu.VMEM((6, ROWS, model_dim), F32),
                pltpu.VMEM((CHUNKS * ROWS, ROWS), F32),
                pltpu.VMEM((CHUNKS * ROWS, ROWS), F32),
                pltpu.VMEM((8, ROWS), F32),
                pltpu.VMEM((8, ROWS), F32),
                pltpu.VMEM((HEADS, head_rows, ROWS), BF16),
                pltpu.VMEM((HEADS, head_rows, ROWS), F32),
                pltpu.VMEM((HEADS, 8, ROWS), F32),
                pltpu.VMEM((HEADS, 8, ROWS), F32),
                pltpu.VMEM((HEADS, 8, ROWS), F32),
                dma((12,)), pltpu.SemaphoreType.REGULAR, dma((10,)), dma((10,)), dma((14,)), dma((14,)),
                dma((2, UNITS + 1)), dma((2, UNITS + 1)), dma((20,)), dma((20,)),
            ],
            compiler_params=pltpu.CompilerParams(collective_id=0, has_side_effects=True, vmem_limit_bytes=64000000),
            name="parallel_block",
        )(x_loc, ln_gamma, w_qkv.transpose(1, 2, 0), w_out, w_up.T, w_down)

    row_spec = P(("data", "tp"), None)
    return jax.shard_map(local_block, mesh=mesh, in_specs=(row_spec, P(None), P(None, "tp", None), P("tp", None, None), P(None, "tp"), P("tp", None)), out_specs=row_spec, check_vma=False)
```

```python
import functools
import math
import jax
import jax.numpy as jnp
from jax import lax
from jax.experimental import pallas as pl
from jax.experimental.pallas import tpu as pltpu
from jax.sharding import PartitionSpec as P

LN_EPS = 1e-6
LANES = 128
ROWS = 256
UNITS = 8
CHUNKS = 2 * UNITS
HEADS = 4
HALF = ROWS // 2
QUARTER = ROWS // 4
F32 = jnp.float32
BF16 = jnp.bfloat16
ROW_MAJOR = (((1,), (0,)), ((), ()))
BY_ROWS = (((1,), (1,)), ((), ()))
BY_COLS = (((0,), (0,)), ((), ()))


def dot(a, b, dims=ROW_MAJOR):
    return lax.dot_general(a, b, dims, preferred_element_type=F32)


def gelu_tanh(v):
    return jax.nn.gelu(v, approximate=True)


def block_kernel(head_dim, head_rows, x_hbm, gamma_ref, wqkv_hbm, wout_hbm, w1_hbm, w2_hbm, y_ref,
                 xg, xn, wqv, wk, wk_t, wout, w1, w2, q_all, k_all, v_all, part, recv, s_even, s_odd, m_even, m_odd, o_t,
                 acc_st, m_st, l_st, m_all,
                 load_sem, pad_sem, wsend, wrecv, gsend, grecv, kvsend, kvrecv, rsend, rrecv):
    me = lax.axis_index("tp")
    core = lax.rem(me, 2)
    chip_x = lax.rem(me // 2, 2)
    chip_y = me // 4
    sib = me + 1 - 2 * core
    x_nbr = me + 2 - 4 * chip_x
    y_nbr = me + 4 - 8 * chip_y
    mesh_id = pl.DeviceIdType.MESH

    def remote(src, dst, send, rcv, dev):
        return pltpu.make_async_remote_copy(src_ref=src, dst_ref=dst, send_sem=send, recv_sem=rcv,
                                            device_id={"tp": dev}, device_id_type=mesh_id)

    barrier = pltpu.get_barrier_semaphore()
    for dev in (x_nbr, y_nbr, sib):
        pl.semaphore_signal(barrier, inc=1, device_id={"tp": dev}, device_id_type=mesh_id)
    loads = [pltpu.make_async_copy(x_hbm.at[pl.ds(half * ROWS, ROWS)], xg.at[half], load_sem.at[half]) for half in (0, 1)]

    pairs = []
    for hh in (0, 1):
        h = 2 * core + hh
        real = pl.ds(0, head_dim)
        pairs += [
            (wqkv_hbm.at[hh, pl.ds(0, head_dim)], wqv.at[0, h, real]),
            (wqkv_hbm.at[hh, pl.ds(head_dim, head_dim)], wk.at[h, real]),
            (wqkv_hbm.at[hh, pl.ds(2 * head_dim, head_dim)], wqv.at[1, h, real]),
            (wout_hbm.at[hh], wout.at[h, real]),
        ]
    pairs += [(w1_hbm, w1.at[core]), (w2_hbm, w2.at[core])]

    pl.semaphore_wait(barrier, 3)

    top, low = pl.ds(0, HALF), pl.ds(HALF, HALF)
    parts = (top, low)

    def diag_copy(src, dst, span, idx, dev):
        return remote(xn.at[src, span], xn.at[dst, span], gsend.at[idx], grecv.at[idx], dev)

    def own(half, j):
        return x_hbm.at[pl.ds(half * ROWS + j * HALF, HALF)]

    g_first = [(remote(own(0, j), xg.at[2 + j, top], gsend.at[j], grecv.at[j], y_nbr), remote(own(1, j), xg.at[2 + j, low], gsend.at[2 + j], grecv.at[2 + j], x_nbr)) for j in (0, 1)]
    g_second = [(remote(own(0, j), xg.at[4 + j, top], gsend.at[4 + j], grecv.at[4 + j], x_nbr), remote(own(1, j), xg.at[4 + j, low], gsend.at[6 + j], grecv.at[6 + j], y_nbr)) for j in (0, 1)]
    g_diag = [(diag_copy(2, 6, top, 8, x_nbr), diag_copy(2, 6, low, 9, y_nbr))]
    for q in (0, 1):
        q_top, q_low = pl.ds(q * QUARTER, QUARTER), pl.ds(HALF + q * QUARTER, QUARTER)
        g_diag.append((diag_copy(3, 7, q_top, 10 + q, x_nbr), diag_copy(3, 7, q_low, 12 + q, y_nbr)))
    g_copies = [cp for group in (g_first, g_second, g_diag) for two in group for cp in two]
    for cp in g_copies[:8] + loads:
        cp.start()
    wqv[:, :, head_rows - 16:, :] = jnp.zeros((2, HEADS, 16, wqv.shape[3]), BF16)
    wk[:, LANES - 64:, :] = jnp.zeros((HEADS, 64, wk.shape[2]), BF16)
    wout[:, head_rows - 16:, :] = jnp.zeros((HEADS, 16, wout.shape[2]), BF16)
    pl.semaphore_signal(pad_sem, inc=1, device_id={"tp": sib}, device_id_type=mesh_id)
    pl.semaphore_wait(pad_sem, 1)
    w_copies = [remote(src, dst, wsend.at[n], wrecv.at[n], sib) for n, (src, dst) in enumerate(pairs)]
    w_loads = [pltpu.make_async_copy(src, dst, load_sem.at[2 + n]) for n, (src, dst) in enumerate(pairs)]
    for cp in w_copies + w_loads:
        cp.start()

    zero_rows = LANES - head_rows

    def clear(unit, _):
        q_all[unit, :, head_rows:, :] = jnp.zeros((HEADS, zero_rows, ROWS), BF16)
        return 0

    lax.fori_loop(0, UNITS, clear, 0)

    def kv_copies(unit):
        return (
            remote(k_all.at[unit], k_all.at[UNITS + unit], kvsend.at[0, unit], kvrecv.at[0, unit], sib),
            remote(v_all.at[unit], v_all.at[UNITS + unit], kvsend.at[1, unit], kvrecv.at[1, unit], sib),
        )

    def normalize(rows):
        rows = rows.astype(F32)
        mean = jnp.mean(rows, axis=-1, keepdims=True)
        cent = rows - mean
        var = jnp.mean(cent * cent, axis=-1, keepdims=True)
        return (cent * lax.rsqrt(var + LN_EPS) * gamma_ref[...][None, :]).astype(BF16)

    last = UNITS - 1

    def last_copies(q):
        span = parts[q]
        return (
            remote(k_all.at[last, :, span], k_all.at[UNITS + last, :, span], kvsend.at[q, last], kvrecv.at[q, last], sib),
            remote(v_all.at[last, :, :, span], v_all.at[UNITS + last, :, :, span], kvsend.at[q, UNITS], kvrecv.at[q, UNITS], sib),
        )

    def project_last(q):
        spans = (pl.ds(q * QUARTER, QUARTER), pl.ds(HALF + q * QUARTER, QUARTER))
        normed = jnp.concatenate([xn[last, span] for span in spans], axis=0)
        keys = dot(normed, wk_t[...])
        for h in range(HEADS):
            k_all[last, h, parts[q]] = keys[:, h * LANES:(h + 1) * LANES].astype(BF16)
        k_copy, v_copy = last_copies(q)
        k_copy.start()
        values = dot(wqv[1].reshape(HEADS * head_rows, -1), normed, BY_ROWS).astype(BF16)
        for h in range(HEADS):
            v_all[last, h, :, parts[q]] = values[h * head_rows:(h + 1) * head_rows]
        v_copy.start()

    def project(unit, _):
        normed = normalize(xg[unit])
        xn[unit] = normed
        return keys_values(unit, normed)

    def keys_values(unit, normed):
        keys = dot(normed, wk_t[...])
        for h in range(HEADS):
            k_all[unit, h] = keys[:, h * LANES:(h + 1) * LANES].astype(BF16)
        k_copy, v_copy = kv_copies(unit)
        k_copy.start()
        values = dot(wqv[1].reshape(HEADS * head_rows, -1), normed, BY_ROWS).astype(BF16)
        for h in range(HEADS):
            v_all[unit, h] = values[h * head_rows:(h + 1) * head_rows]
        v_copy.start()
        return 0

    def project_queries(unit, _):
        queries = dot(wqv[0].reshape(HEADS * head_rows, -1), xn[unit], BY_ROWS).astype(BF16)
        for h in range(HEADS):
            q_all[unit, h, :head_rows] = queries[h * head_rows:(h + 1) * head_rows]
        return 0

    def project_both(unit, _):
        project(unit, 0)
        return project_queries(unit, 0)

    def mlp(unit, _):
        rows = xn[unit]
        total = None
        for s in (0, 1):
            hidden = gelu_tanh(dot(rows, w1[s], BY_ROWS)).astype(BF16)
            term = dot(hidden, w2[s])
            total = term if total is None else total + term
        part[unit] = total
        return 0

    def kv_wait(unit, _):
        for cp in kv_copies(unit):
            cp.wait()
        return 0

    exp_scale = (head_dim ** -0.5) * math.log2(math.e)
    groups = ROWS // 8

    def chunks_of(*units):
        return list(units) + [UNITS + u for u in units]


    def score_chunk(n, c, h, q, s_ref):
        s = dot(k_all[c, h], q)
        s_ref[pl.ds(n * ROWS, ROWS), :] = s
        return jnp.max(s.reshape(groups, 8, ROWS), axis=0)

    def finish(chunks, h, s_ref, m_ref, unit_n, h_n, s_next, m_next):
        q_n = q_all[unit_n, h_n]
        m = jnp.max(m_ref[...], axis=0, keepdims=True)
        acc = None
        total = None
        m_n = None
        for n, c in enumerate(chunks):
            mc = score_chunk(n, c, h_n, q_n, s_next)
            m_n = mc if m_n is None else jnp.maximum(m_n, mc)
            e = jnp.exp2((s_ref[pl.ds(n * ROWS, ROWS), :] - m) * exp_scale)
            tc = jnp.sum(e.reshape(groups, 8, ROWS), axis=0)
            total = tc if total is None else total + tc
            pv = dot(v_all[c, h], e.astype(BF16))
            acc = pv if acc is None else acc + pv
        m_next[...] = m_n
        return m, jnp.sum(total, axis=0, keepdims=True), acc

    def attend(count, unit_of, chunks, emit, after):
        q = q_all[unit_of(0), 0]
        m = None
        for n, c in enumerate(chunks):
            mc = score_chunk(n, c, 0, q, s_even)
            m = mc if m is None else jnp.maximum(m, mc)
        m_even[...] = m

        def one(i, _):
            unit = unit_of(i)
            unit_next = unit_of(lax.rem(i + 1, count))

            def pair(p, _):
                emit(i, 2 * p, *finish(chunks, 2 * p, s_even, m_even, unit, 2 * p + 1, s_odd, m_odd))
                follow = unit + p * (unit_next - unit)
                emit(i, 2 * p + 1, *finish(chunks, 2 * p + 1, s_odd, m_odd, follow, 2 - 2 * p, s_even, m_even))
                return 0

            lax.fori_loop(0, 2, pair, 0)
            after(i, unit)
            return 0

        lax.fori_loop(0, count, one, 0)

    def emit_state(i, h, m, total, acc):
        m_st[h] = jnp.broadcast_to(m, m_st.shape[1:])
        l_st[h] = jnp.broadcast_to(total, l_st.shape[1:])
        acc_st[h] = acc

    def more_chunks(pieces, emit, s_ref, before_values=None):
        size = ROWS if pieces[0][1] is None else HALF

        def rows_of(h, n):
            return pl.ds((h * len(pieces) + n) * size, size)

        for h in range(HEADS):
            q = q_all[2, h]
            m = None
            for n, (c, part_no) in enumerate(pieces):
                s = dot(k_all[c, h] if part_no is None else k_all[c, h, parts[part_no]], q)
                s_ref[rows_of(h, n), :] = s
                mc = jnp.max(s.reshape(size // 8, 8, ROWS), axis=0)
                m = mc if m is None else jnp.maximum(m, mc)
            m_all[h] = m
        if before_values is not None:
            before_values()
        for h in range(HEADS):
            m = jnp.max(m_all[h], axis=0, keepdims=True)
            total = None
            acc = None
            for n, (c, part_no) in enumerate(pieces):
                e = jnp.exp2((s_ref[rows_of(h, n), :] - m) * exp_scale)
                tc = jnp.sum(e.reshape(size // 8, 8, ROWS), axis=0)
                total = tc if total is None else total + tc
                v = v_all[c, h] if part_no is None else v_all[c, h, :, parts[part_no]]
                pv = dot(v, e.astype(BF16))
                acc = pv if acc is None else acc + pv
            emit(0, h, m, jnp.sum(total, axis=0, keepdims=True), acc)

    def joined(h, m, total, acc):
        m_old = m_st[h][:1]
        high = jnp.maximum(m, m_old)
        a_new = jnp.exp2((m - high) * exp_scale)
        a_old = jnp.exp2((m_old - high) * exp_scale)
        return high, total * a_new + l_st[h][:1] * a_old, acc * a_new + acc_st[h] * a_old

    def emit_joined(i, h, m, total, acc):
        emit_state(i, h, *joined(h, m, total, acc))

    def emit_last(i, h, m, total, acc):
        emit_out(i, h, *joined(h, m, total, acc))

    def emit_out(i, h, m, total, acc):
        o_t[h] = (acc / total).astype(BF16)

    def add_heads(unit):
        part[unit] += dot(o_t[...].reshape(HEADS * head_rows, ROWS), wout[...].reshape(HEADS * head_rows, -1), BY_COLS)

    def reduce_copy(src, dst, start, size, sem, dev):
        span = pl.ds(start, size)
        return remote(part.at[src, span], recv.at[dst, span], rsend.at[sem], rrecv.at[sem], dev)

    r_first = [(reduce_copy(2 + j, j, 0, HALF, 2 * j, y_nbr), reduce_copy(2 + j, j, HALF, HALF, 2 * j + 1, x_nbr)) for j in (0, 1)]
    quarters = (0, 2, 1, 3)

    def quarter_copies(src, dst, sem, first, second):
        return [reduce_copy(src, dst, n * QUARTER, QUARTER, sem + n, first if n < 2 else second) for n in range(4)]

    r_join = [quarter_copies(6 + j, 2 + j, 4 + 4 * j, y_nbr, x_nbr) for j in (0, 1)]
    r_last = [quarter_copies(4 + j, 4 + j, 12 + 4 * j, x_nbr, y_nbr) for j in (0, 1)]

    for cp in loads + w_loads:
        cp.wait()
    for cp in w_copies:
        cp.wait_recv()
    for h in range(HEADS):
        wk_t[:, h * LANES:(h + 1) * LANES] = jnp.transpose(wk[h])
    lax.fori_loop(0, 2, project_both, 0)
    lax.fori_loop(0, 2, mlp, 0)
    for j in (0, 1):
        for cp in g_first[j]:
            cp.wait_recv()
        project_both(2 + j, 0)
        for cp in g_diag[j]:
            cp.start()

    def send_last():
        for cp in g_diag[2]:
            cp.start()

    pl.when(core == 0)(send_last)
    lax.fori_loop(0, 4, kv_wait, 0)
    attend(1, lambda i: 2, chunks_of(0, 1, 2, 3), emit_state, lambda i, unit: None)
    lax.fori_loop(2, 4, mlp, 0)
    for j in (0, 1):
        for cp in g_second[j]:
            cp.wait_recv()
    lax.fori_loop(4, 6, project_both, 0)
    lax.fori_loop(4, 6, kv_wait, 0)
    more_chunks([(c, None) for c in chunks_of(4, 5)], emit_joined, s_even)
    for cp in g_diag[0]:
        cp.wait_recv()
    keys_values(6, xn[6])
    project_queries(6, 0)
    pl.when(core == 1)(send_last)
    kv_wait(6, 0)
    more_chunks([(c, None) for c in chunks_of(6)], emit_joined, s_odd)
    for cp in g_diag[1]:
        cp.wait_recv()
    project_last(0)
    more_chunks([(last, 0)], emit_joined, s_even)
    for cp in g_diag[2]:
        cp.wait_recv()
    project_last(1)
    for cp in last_copies(0):
        cp.wait()
    more_chunks([(last, 1), (UNITS + last, 0)], emit_joined, s_odd)
    k_last, v_last = last_copies(1)
    k_last.wait()
    more_chunks([(UNITS + last, 1)], emit_last, s_even, before_values=v_last.wait)
    add_heads(2)
    for cp in r_first[0]:
        cp.start()
    project_queries(last, 0)

    def join(j):
        for n in quarters:
            span = pl.ds(n * QUARTER, QUARTER)
            r_join[j][n].wait_recv()
            part[4 + j, span, :] += recv[2 + j, span, :]
            r_last[j][n].start()

    def later_unit(i):
        p = (i + 1) // 2
        return 2 * (1 + 2 * ((p + 2) // 3) - p // 2 - 2 * (p // 3)) + lax.rem(i + 1, 2)

    def after_later(i, unit):
        @pl.when((i >= 1) & (i <= 4))
        def _():
            mlp(unit, 0)

        add_heads(unit)

        @pl.when(i == 0)
        def _():
            for cp in r_first[1]:
                cp.start()

        for step in (0, 1):
            @pl.when(i == step + 1)
            def _():
                for n in quarters:
                    r_join[step][n].start()

        @pl.when(i == 4)
        def _():
            join(0)

    attend(7, later_unit, list(range(CHUNKS)), emit_out, after_later)
    join(1)
    for j in (0, 1):
        for half in (0, 1):
            r_first[j][half].wait_recv()
            part[half, parts[j], :] += xg[half, parts[j], :].astype(F32) + recv[j, parts[half], :]
    for j in (0, 1):
        for n in quarters:
            half, start = n // 2, j * HALF + (n % 2) * QUARTER
            r_last[j][n].wait_recv()
            total = part[half, pl.ds(start, QUARTER), :] + recv[4 + j, pl.ds(n * QUARTER, QUARTER), :]
            y_ref[pl.ds(half * ROWS + start, QUARTER), :] = total.astype(BF16)
    for cp in g_copies + w_copies:
        cp.wait_send()
    for group in r_first + r_join + r_last:
        for cp in group:
            cp.wait_send()


def solution(mesh):
    def local_block(x_loc, ln_gamma, w_qkv, w_out, w_up, w_down):
        model_dim = x_loc.shape[1]
        head_dim = w_qkv.shape[2] // 3
        ff = w_up.shape[1]
        head_rows = -(-head_dim // 16) * 16
        hbm = pl.BlockSpec(memory_space=pltpu.HBM)
        vmem = pl.BlockSpec(memory_space=pltpu.VMEM)
        dma = pltpu.SemaphoreType.DMA
        return pl.pallas_call(
            functools.partial(block_kernel, head_dim, head_rows),
            out_shape=pltpu.VMEM(x_loc.shape, BF16),
            in_specs=[hbm, vmem, hbm, hbm, hbm, hbm],
            out_specs=vmem,
            scratch_shapes=[
                pltpu.VMEM((UNITS - 2, ROWS, model_dim), BF16),
                pltpu.VMEM((UNITS, ROWS, model_dim), BF16),
                pltpu.VMEM((2, HEADS, head_rows, model_dim), BF16),
                pltpu.VMEM((HEADS, LANES, model_dim), BF16),
                pltpu.VMEM((model_dim, HEADS * LANES), BF16),
                pltpu.VMEM((HEADS, head_rows, model_dim), BF16),
                pltpu.VMEM((2, ff, model_dim), BF16),
                pltpu.VMEM((2, ff, model_dim), BF16),
                pltpu.VMEM((UNITS, HEADS, LANES, ROWS), BF16),
                pltpu.VMEM((CHUNKS, HEADS, ROWS, LANES), BF16),
                pltpu.VMEM((CHUNKS, HEADS, head_rows, ROWS), BF16),
                pltpu.VMEM((UNITS, ROWS, model_dim), F32),
                pltpu.VMEM((6, ROWS, model_dim), F32),
                pltpu.VMEM((CHUNKS * ROWS, ROWS), F32),
                pltpu.VMEM((CHUNKS * ROWS, ROWS), F32),
                pltpu.VMEM((8, ROWS), F32),
                pltpu.VMEM((8, ROWS), F32),
                pltpu.VMEM((HEADS, head_rows, ROWS), BF16),
                pltpu.VMEM((HEADS, head_rows, ROWS), F32),
                pltpu.VMEM((HEADS, 8, ROWS), F32),
                pltpu.VMEM((HEADS, 8, ROWS), F32),
                pltpu.VMEM((HEADS, 8, ROWS), F32),
                dma((12,)), pltpu.SemaphoreType.REGULAR, dma((10,)), dma((10,)), dma((14,)), dma((14,)),
                dma((2, UNITS + 1)), dma((2, UNITS + 1)), dma((20,)), dma((20,)),
            ],
            compiler_params=pltpu.CompilerParams(collective_id=0, has_side_effects=True, vmem_limit_bytes=64000000),
            name="parallel_block",
        )(x_loc, ln_gamma, w_qkv.transpose(1, 2, 0), w_out, w_up.T, w_down)

    row_spec = P(("data", "tp"), None)
    return jax.shard_map(local_block, mesh=mesh, in_specs=(row_spec, P(None), P(None, "tp", None), P("tp", None, None), P(None, "tp"), P("tp", None)), out_specs=row_spec, check_vma=False)
```

```python
import functools
import math
import jax
import jax.numpy as jnp
from jax import lax
from jax.experimental import pallas as pl
from jax.experimental.pallas import tpu as pltpu
from jax.sharding import PartitionSpec as P

LN_EPS = 1e-6
LANES = 128
ROWS = 256
UNITS = 8
CHUNKS = 2 * UNITS
HEADS = 4
HALF = ROWS // 2
QUARTER = ROWS // 4
F32 = jnp.float32
BF16 = jnp.bfloat16
ROW_MAJOR = (((1,), (0,)), ((), ()))
BY_ROWS = (((1,), (1,)), ((), ()))
BY_COLS = (((0,), (0,)), ((), ()))


def dot(a, b, dims=ROW_MAJOR):
    return lax.dot_general(a, b, dims, preferred_element_type=F32)


def gelu_tanh(v):
    return jax.nn.gelu(v, approximate=True)


def block_kernel(head_dim, head_rows, x_hbm, gamma_ref, wqkv_hbm, wout_hbm, w1_hbm, w2_hbm, y_ref,
                 xg, xn, wqv, wk, wk_t, wout, w1, w2, q_all, k_all, v_all, part, recv, s_even, s_odd, m_even, m_odd, o_t,
                 acc_st, m_st, l_st, m_all,
                 load_sem, pad_sem, wsend, wrecv, gsend, grecv, kvsend, kvrecv, rsend, rrecv):
    me = lax.axis_index("tp")
    core = lax.rem(me, 2)
    chip_x = lax.rem(me // 2, 2)
    chip_y = me // 4
    sib = me + 1 - 2 * core
    x_nbr = me + 2 - 4 * chip_x
    y_nbr = me + 4 - 8 * chip_y
    mesh_id = pl.DeviceIdType.MESH

    def remote(src, dst, send, rcv, dev):
        return pltpu.make_async_remote_copy(src_ref=src, dst_ref=dst, send_sem=send, recv_sem=rcv,
                                            device_id={"tp": dev}, device_id_type=mesh_id)

    barrier = pltpu.get_barrier_semaphore()
    for dev in (x_nbr, y_nbr, sib):
        pl.semaphore_signal(barrier, inc=1, device_id={"tp": dev}, device_id_type=mesh_id)
    loads = [pltpu.make_async_copy(x_hbm.at[pl.ds(half * ROWS, ROWS)], xg.at[half], load_sem.at[half]) for half in (0, 1)]

    pairs = []
    for hh in (0, 1):
        h = 2 * core + hh
        real = pl.ds(0, head_dim)
        pairs += [
            (wqkv_hbm.at[hh, pl.ds(0, head_dim)], wqv.at[0, h, real]),
            (wqkv_hbm.at[hh, pl.ds(head_dim, head_dim)], wk.at[h, real]),
            (wqkv_hbm.at[hh, pl.ds(2 * head_dim, head_dim)], wqv.at[1, h, real]),
            (wout_hbm.at[hh], wout.at[h, real]),
        ]
    pairs += [(w1_hbm, w1.at[core]), (w2_hbm, w2.at[core])]

    pl.semaphore_wait(barrier, 3)

    top, low = pl.ds(0, HALF), pl.ds(HALF, HALF)
    parts = (top, low)

    def diag_copy(src, dst, span, idx, dev):
        return remote(xn.at[src, span], xn.at[dst, span], gsend.at[idx], grecv.at[idx], dev)

    def own(half, j):
        return x_hbm.at[pl.ds(half * ROWS + j * HALF, HALF)]

    g_first = [(remote(own(0, j), xg.at[2 + j, top], gsend.at[j], grecv.at[j], y_nbr), remote(own(1, j), xg.at[2 + j, low], gsend.at[2 + j], grecv.at[2 + j], x_nbr)) for j in (0, 1)]
    g_second = [(remote(own(0, j), xg.at[4 + j, top], gsend.at[4 + j], grecv.at[4 + j], x_nbr), remote(own(1, j), xg.at[4 + j, low], gsend.at[6 + j], grecv.at[6 + j], y_nbr)) for j in (0, 1)]
    g_diag = [(diag_copy(2, 6, top, 8, x_nbr), diag_copy(2, 6, low, 9, y_nbr))]
    for q in (0, 1):
        q_top, q_low = pl.ds(q * QUARTER, QUARTER), pl.ds(HALF + q * QUARTER, QUARTER)
        g_diag.append((diag_copy(3, 7, q_top, 10 + q, x_nbr), diag_copy(3, 7, q_low, 12 + q, y_nbr)))
    g_copies = [cp for group in (g_first, g_second, g_diag) for two in group for cp in two]
    for cp in g_copies[:8] + loads:
        cp.start()
    wqv[:, :, head_rows - 16:, :] = jnp.zeros((2, HEADS, 16, wqv.shape[3]), BF16)
    wk[:, LANES - 64:, :] = jnp.zeros((HEADS, 64, wk.shape[2]), BF16)
    wout[:, head_rows - 16:, :] = jnp.zeros((HEADS, 16, wout.shape[2]), BF16)
    pl.semaphore_signal(pad_sem, inc=1, device_id={"tp": sib}, device_id_type=mesh_id)
    pl.semaphore_wait(pad_sem, 1)
    w_copies = [remote(src, dst, wsend.at[n], wrecv.at[n], sib) for n, (src, dst) in enumerate(pairs)]
    w_loads = [pltpu.make_async_copy(src, dst, load_sem.at[2 + n]) for n, (src, dst) in enumerate(pairs)]
    for cp in w_copies + w_loads:
        cp.start()

    zero_rows = LANES - head_rows

    def clear(unit, _):
        q_all[unit, :, head_rows:, :] = jnp.zeros((HEADS, zero_rows, ROWS), BF16)
        return 0

    lax.fori_loop(0, UNITS, clear, 0)

    def kv_copies(unit):
        return (
            remote(k_all.at[unit], k_all.at[UNITS + unit], kvsend.at[0, unit], kvrecv.at[0, unit], sib),
            remote(v_all.at[unit], v_all.at[UNITS + unit], kvsend.at[1, unit], kvrecv.at[1, unit], sib),
        )

    def normalize(rows):
        rows = rows.astype(F32)
        mean = jnp.mean(rows, axis=-1, keepdims=True)
        cent = rows - mean
        var = jnp.mean(cent * cent, axis=-1, keepdims=True)
        return (cent * lax.rsqrt(var + LN_EPS) * gamma_ref[...][None, :]).astype(BF16)

    last = UNITS - 1

    def last_copies(q):
        span = parts[q]
        return (
            remote(k_all.at[last, :, span], k_all.at[UNITS + last, :, span], kvsend.at[q, last], kvrecv.at[q, last], sib),
            remote(v_all.at[last, :, :, span], v_all.at[UNITS + last, :, :, span], kvsend.at[q, UNITS], kvrecv.at[q, UNITS], sib),
        )

    def project_last(q):
        spans = (pl.ds(q * QUARTER, QUARTER), pl.ds(HALF + q * QUARTER, QUARTER))
        normed = jnp.concatenate([xn[last, span] for span in spans], axis=0)
        keys = dot(normed, wk_t[...])
        for h in range(HEADS):
            k_all[last, h, parts[q]] = keys[:, h * LANES:(h + 1) * LANES].astype(BF16)
        k_copy, v_copy = last_copies(q)
        k_copy.start()
        values = dot(wqv[1].reshape(HEADS * head_rows, -1), normed, BY_ROWS).astype(BF16)
        for h in range(HEADS):
            v_all[last, h, :, parts[q]] = values[h * head_rows:(h + 1) * head_rows]
        v_copy.start()

    def project(unit, _):
        normed = normalize(xg[unit])
        xn[unit] = normed
        return keys_values(unit, normed)

    def keys_values(unit, normed):
        keys = dot(normed, wk_t[...])
        for h in range(HEADS):
            k_all[unit, h] = keys[:, h * LANES:(h + 1) * LANES].astype(BF16)
        k_copy, v_copy = kv_copies(unit)
        k_copy.start()
        values = dot(wqv[1].reshape(HEADS * head_rows, -1), normed, BY_ROWS).astype(BF16)
        for h in range(HEADS):
            v_all[unit, h] = values[h * head_rows:(h + 1) * head_rows]
        v_copy.start()
        return 0

    def project_queries(unit, _):
        queries = dot(wqv[0].reshape(HEADS * head_rows, -1), xn[unit], BY_ROWS).astype(BF16)
        for h in range(HEADS):
            q_all[unit, h, :head_rows] = queries[h * head_rows:(h + 1) * head_rows]
        return 0

    def project_both(unit, _):
        project(unit, 0)
        return project_queries(unit, 0)

    def mlp(unit, _):
        rows = xn[unit]
        total = None
        for s in (0, 1):
            hidden = gelu_tanh(dot(rows, w1[s], BY_ROWS)).astype(BF16)
            term = dot(hidden, w2[s])
            total = term if total is None else total + term
        part[unit] = total
        return 0

    def kv_wait(unit, _):
        for cp in kv_copies(unit):
            cp.wait()
        return 0

    exp_scale = (head_dim ** -0.5) * math.log2(math.e)
    groups = ROWS // 8

    def chunks_of(*units):
        return list(units) + [UNITS + u for u in units]


    def score_chunk(n, c, h, q, s_ref):
        s = dot(k_all[c, h], q)
        s_ref[pl.ds(n * ROWS, ROWS), :] = s
        return jnp.max(s.reshape(groups, 8, ROWS), axis=0)

    def finish(chunks, h, s_ref, m_ref, unit_n, h_n, s_next, m_next):
        q_n = q_all[unit_n, h_n]
        m = jnp.max(m_ref[...], axis=0, keepdims=True)
        acc = None
        total = None
        m_n = None
        for n, c in enumerate(chunks):
            mc = score_chunk(n, c, h_n, q_n, s_next)
            m_n = mc if m_n is None else jnp.maximum(m_n, mc)
            e = jnp.exp2((s_ref[pl.ds(n * ROWS, ROWS), :] - m) * exp_scale)
            tc = jnp.sum(e.reshape(groups, 8, ROWS), axis=0)
            total = tc if total is None else total + tc
            pv = dot(v_all[c, h], e.astype(BF16))
            acc = pv if acc is None else acc + pv
        m_next[...] = m_n
        return m, jnp.sum(total, axis=0, keepdims=True), acc

    def attend(count, unit_of, chunks, emit, after):
        q = q_all[unit_of(0), 0]
        m = None
        for n, c in enumerate(chunks):
            mc = score_chunk(n, c, 0, q, s_even)
            m = mc if m is None else jnp.maximum(m, mc)
        m_even[...] = m

        def one(i, _):
            unit = unit_of(i)
            unit_next = unit_of(lax.rem(i + 1, count))

            def pair(p, _):
                emit(i, 2 * p, *finish(chunks, 2 * p, s_even, m_even, unit, 2 * p + 1, s_odd, m_odd))
                follow = unit + p * (unit_next - unit)
                emit(i, 2 * p + 1, *finish(chunks, 2 * p + 1, s_odd, m_odd, follow, 2 - 2 * p, s_even, m_even))
                return 0

            lax.fori_loop(0, 2, pair, 0)
            after(i, unit)
            return 0

        lax.fori_loop(0, count, one, 0)

    def emit_state(i, h, m, total, acc):
        m_st[h] = jnp.broadcast_to(m, m_st.shape[1:])
        l_st[h] = jnp.broadcast_to(total, l_st.shape[1:])
        acc_st[h] = acc

    def more_chunks(pieces, emit, s_ref, before_values=None):
        size = ROWS if pieces[0][1] is None else HALF

        def rows_of(h, n):
            return pl.ds((h * len(pieces) + n) * size, size)

        for h in range(HEADS):
            q = q_all[2, h]
            m = None
            for n, (c, part_no) in enumerate(pieces):
                s = dot(k_all[c, h] if part_no is None else k_all[c, h, parts[part_no]], q)
                s_ref[rows_of(h, n), :] = s
                mc = jnp.max(s.reshape(size // 8, 8, ROWS), axis=0)
                m = mc if m is None else jnp.maximum(m, mc)
            m_all[h] = m
        if before_values is not None:
            before_values()
        for h in range(HEADS):
            m = jnp.max(m_all[h], axis=0, keepdims=True)
            total = None
            acc = None
            for n, (c, part_no) in enumerate(pieces):
                e = jnp.exp2((s_ref[rows_of(h, n), :] - m) * exp_scale)
                tc = jnp.sum(e.reshape(size // 8, 8, ROWS), axis=0)
                total = tc if total is None else total + tc
                v = v_all[c, h] if part_no is None else v_all[c, h, :, parts[part_no]]
                pv = dot(v, e.astype(BF16))
                acc = pv if acc is None else acc + pv
            emit(0, h, m, jnp.sum(total, axis=0, keepdims=True), acc)

    def joined(h, m, total, acc):
        m_old = m_st[h][:1]
        high = jnp.maximum(m, m_old)
        a_new = jnp.exp2((m - high) * exp_scale)
        a_old = jnp.exp2((m_old - high) * exp_scale)
        return high, total * a_new + l_st[h][:1] * a_old, acc * a_new + acc_st[h] * a_old

    def emit_joined(i, h, m, total, acc):
        emit_state(i, h, *joined(h, m, total, acc))

    def emit_last(i, h, m, total, acc):
        emit_out(i, h, *joined(h, m, total, acc))

    def emit_out(i, h, m, total, acc):
        o_t[h] = (acc / total).astype(BF16)

    def add_heads(unit):
        part[unit] += dot(o_t[...].reshape(HEADS * head_rows, ROWS), wout[...].reshape(HEADS * head_rows, -1), BY_COLS)

    def reduce_copy(src, dst, start, size, sem, dev):
        span = pl.ds(start, size)
        return remote(part.at[src, span], recv.at[dst, span], rsend.at[sem], rrecv.at[sem], dev)

    r_first = [(reduce_copy(2 + j, j, 0, HALF, 2 * j, y_nbr), reduce_copy(2 + j, j, HALF, HALF, 2 * j + 1, x_nbr)) for j in (0, 1)]
    quarters = (0, 2, 1, 3)

    def quarter_copies(src, dst, sem, first, second):
        return [reduce_copy(src, dst, n * QUARTER, QUARTER, sem + n, first if n < 2 else second) for n in range(4)]

    r_join = [quarter_copies(6 + j, 2 + j, 4 + 4 * j, y_nbr, x_nbr) for j in (0, 1)]
    r_last = [quarter_copies(4 + j, 4 + j, 12 + 4 * j, x_nbr, y_nbr) for j in (0, 1)]

    for cp in loads + w_loads:
        cp.wait()
    for cp in w_copies:
        cp.wait_recv()
    for h in range(HEADS):
        wk_t[:, h * LANES:(h + 1) * LANES] = jnp.transpose(wk[h])
    lax.fori_loop(0, 2, project_both, 0)
    lax.fori_loop(0, 2, mlp, 0)
    for j in (0, 1):
        for cp in g_first[j]:
            cp.wait_recv()
        project_both(2 + j, 0)
        for cp in g_diag[j]:
            cp.start()

    def send_last():
        for cp in g_diag[2]:
            cp.start()

    pl.when(core == 0)(send_last)
    lax.fori_loop(0, 4, kv_wait, 0)
    attend(1, lambda i: 2, chunks_of(0, 1, 2, 3), emit_state, lambda i, unit: None)
    lax.fori_loop(2, 4, mlp, 0)
    for j in (0, 1):
        for cp in g_second[j]:
            cp.wait_recv()
    lax.fori_loop(4, 6, project_both, 0)
    lax.fori_loop(4, 6, kv_wait, 0)
    more_chunks([(c, None) for c in chunks_of(4, 5)], emit_joined, s_even)
    for cp in g_diag[0]:
        cp.wait_recv()
    keys_values(6, xn[6])
    project_queries(6, 0)
    pl.when(core == 1)(send_last)
    kv_wait(6, 0)
    more_chunks([(c, None) for c in chunks_of(6)], emit_joined, s_odd)
    for cp in g_diag[1]:
        cp.wait_recv()
    project_last(0)
    more_chunks([(last, 0)], emit_joined, s_even)
    for cp in g_diag[2]:
        cp.wait_recv()
    project_last(1)
    for cp in last_copies(0):
        cp.wait()
    more_chunks([(last, 1), (UNITS + last, 0)], emit_joined, s_odd)
    k_last, v_last = last_copies(1)
    k_last.wait()
    more_chunks([(UNITS + last, 1)], emit_last, s_even, before_values=v_last.wait)
    add_heads(2)
    for cp in r_first[0]:
        cp.start()
    project_queries(last, 0)

    def join(j):
        for n in quarters:
            span = pl.ds(n * QUARTER, QUARTER)
            r_join[j][n].wait_recv()
            part[4 + j, span, :] += recv[2 + j, span, :]
            if j == 1 and n % 2 == 1:
                pl.when(core == 0)(r_last[j][n].start)
            else:
                r_last[j][n].start()

    def later_unit(i):
        p = (i + 1) // 2
        return 2 * (1 + 2 * ((p + 2) // 3) - p // 2 - 2 * (p // 3)) + lax.rem(i + 1, 2)

    def after_later(i, unit):
        @pl.when((i >= 1) & (i <= 4))
        def _():
            mlp(unit, 0)

        add_heads(unit)

        @pl.when(i == 0)
        def _():
            for cp in r_first[1]:
                cp.start()

        for step in (0, 1):
            @pl.when(i == step + 1)
            def _():
                for n in quarters:
                    r_join[step][n].start()

        @pl.when(i == 4)
        def _():
            join(0)

    attend(7, later_unit, list(range(CHUNKS)), emit_out, after_later)
    join(1)
    for j in (0, 1):
        for half in (0, 1):
            r_first[j][half].wait_recv()
            part[half, parts[j], :] += xg[half, parts[j], :].astype(F32) + recv[j, parts[half], :]
    for j in (0, 1):
        for n in quarters:
            half, start = n // 2, j * HALF + (n % 2) * QUARTER
            r_last[j][n].wait_recv()
            if j == 1 and n % 2 == 0:
                pl.when(core == 1)(r_last[j][n + 1].start)
            total = part[half, pl.ds(start, QUARTER), :] + recv[4 + j, pl.ds(n * QUARTER, QUARTER), :]
            y_ref[pl.ds(half * ROWS + start, QUARTER), :] = total.astype(BF16)
    for cp in g_copies + w_copies:
        cp.wait_send()
    for group in r_first + r_join + r_last:
        for cp in group:
            cp.wait_send()


def solution(mesh):
    def local_block(x_loc, ln_gamma, w_qkv, w_out, w_up, w_down):
        model_dim = x_loc.shape[1]
        head_dim = w_qkv.shape[2] // 3
        ff = w_up.shape[1]
        head_rows = -(-head_dim // 16) * 16
        hbm = pl.BlockSpec(memory_space=pltpu.HBM)
        vmem = pl.BlockSpec(memory_space=pltpu.VMEM)
        dma = pltpu.SemaphoreType.DMA
        return pl.pallas_call(
            functools.partial(block_kernel, head_dim, head_rows),
            out_shape=pltpu.VMEM(x_loc.shape, BF16),
            in_specs=[hbm, vmem, hbm, hbm, hbm, hbm],
            out_specs=vmem,
            scratch_shapes=[
                pltpu.VMEM((UNITS - 2, ROWS, model_dim), BF16),
                pltpu.VMEM((UNITS, ROWS, model_dim), BF16),
                pltpu.VMEM((2, HEADS, head_rows, model_dim), BF16),
                pltpu.VMEM((HEADS, LANES, model_dim), BF16),
                pltpu.VMEM((model_dim, HEADS * LANES), BF16),
                pltpu.VMEM((HEADS, head_rows, model_dim), BF16),
                pltpu.VMEM((2, ff, model_dim), BF16),
                pltpu.VMEM((2, ff, model_dim), BF16),
                pltpu.VMEM((UNITS, HEADS, LANES, ROWS), BF16),
                pltpu.VMEM((CHUNKS, HEADS, ROWS, LANES), BF16),
                pltpu.VMEM((CHUNKS, HEADS, head_rows, ROWS), BF16),
                pltpu.VMEM((UNITS, ROWS, model_dim), F32),
                pltpu.VMEM((6, ROWS, model_dim), F32),
                pltpu.VMEM((CHUNKS * ROWS, ROWS), F32),
                pltpu.VMEM((CHUNKS * ROWS, ROWS), F32),
                pltpu.VMEM((8, ROWS), F32),
                pltpu.VMEM((8, ROWS), F32),
                pltpu.VMEM((HEADS, head_rows, ROWS), BF16),
                pltpu.VMEM((HEADS, head_rows, ROWS), F32),
                pltpu.VMEM((HEADS, 8, ROWS), F32),
                pltpu.VMEM((HEADS, 8, ROWS), F32),
                pltpu.VMEM((HEADS, 8, ROWS), F32),
                dma((12,)), pltpu.SemaphoreType.REGULAR, dma((10,)), dma((10,)), dma((14,)), dma((14,)),
                dma((2, UNITS + 1)), dma((2, UNITS + 1)), dma((20,)), dma((20,)),
            ],
            compiler_params=pltpu.CompilerParams(collective_id=0, has_side_effects=True, vmem_limit_bytes=64000000),
            name="parallel_block",
        )(x_loc, ln_gamma, w_qkv.transpose(1, 2, 0), w_out, w_up.T, w_down)

    row_spec = P(("data", "tp"), None)
    return jax.shard_map(local_block, mesh=mesh, in_specs=(row_spec, P(None), P(None, "tp", None), P("tp", None, None), P(None, "tp"), P("tp", None)), out_specs=row_spec, check_vma=False)
```
